256 devices in a mesh: groups: 2 (over y), gx: 128 (over z, x, core).
Axes of the slice: x: 4, y: 2, z: 16, core: 2. Of those that a mesh axis runs over, the one named last changes fastest.
The devices are a block of a 4x16x16 slice.
Arguments:
- stream_in: bfloat16 [256, 8192], P(('groups', 'gx')), parts along dimension 0, may hold values from -6 to 6
- query: bfloat16 [256, 8192], P(('groups', 'gx')), parts along dimension 0, may hold values from -4.5 to 4.5
- key_new: bfloat16 [256, 1024], P(('groups', 'gx')), parts along dimension 0, may hold values from -4.5 to 4.5
- value_new: bfloat16 [256, 1024], P(('groups', 'gx')), parts along dimension 0, may hold values from -6 to 6
- key_cache: bfloat16 [256, 128, 1024], P(('groups', 'gx')), parts along dimension 0, may hold values from -6 to 6
- value_cache: bfloat16 [256, 128, 1024], P(('groups', 'gx')), parts along dimension 0, may hold values from -6 to 6
- lengths: int32 [256], P(('groups', 'gx')), parts along dimension 0, may hold values from 1 to 128, as said below
- route_ids: int32 [256, 2], P(('groups', 'gx')), parts along dimension 0, may hold values from 0 to 3, as said below
- route_scores: float32 [256, 2], P(('groups', 'gx')), parts along dimension 0, may hold values from -6 to 6
- out_weight: bfloat16 [8192, 8192], P(None, 'gx'), may hold values from -0.0625 to 0.0625
- norm_gain: float32 [8192], replicated, may hold values from 0.1 to 1.9
- gate_weight: bfloat16 [2, 131072, 896], P(None, 'gx'), may hold values from -0.0625 to 0.0625
- up_weight: bfloat16 [2, 131072, 896], P(None, 'gx'), may hold values from -0.0625 to 0.0625
- down_weight: bfloat16 [2, 114688, 1024], P(None, 'gx'), may hold values from -0.046875 to 0.046875
Outputs:
- layer_out: bfloat16 [256, 8192], P(('groups', 'gx')), parts along dimension 0
The draws below stay inside these ranges and needn't reach their ends.
There are 2 independent parts, one for each index of `groups`. The reference program is written for one: setup_inputs(seed, part) draws one part's arguments, and reference() takes and returns one part's arrays. A program takes and returns all parts, laid end to end along the dimension named above; an argument that names none is the same for every part. Nothing has to cross between parts.
Inputs may be any that keep to these rules, and one draw needn't show every extreme that they name: `lengths`: 1 to 128; some sequence fills all 128 slots. `route_ids`: each row names two different experts of 0 to 3; in one replica's batch each of the experts 0 and 1 is named by at most 80 sequences, and one of them by exactly 80.
All inputs are finite; a program needn't handle non-finite values.
Results may differ from the reference program's by a relative error of at most 0.0095.
Values may be sent and summed in bfloat16 or wider, within the bound.
A program may use at most 64 MiB of HBM per device.

```python
import jax
import jax.numpy as jnp
from jax import lax

D = 8192
NH = 64
KVH = 8
HS = 128
H = 14336
RESIDENT = 2
MSPLIT = 8
CTX = 128
HSPLIT = 16
BATCH = 128


def shared_heads(key):
    base = jax.random.fold_in(key, 71)
    key_q, key_k = jax.random.split(base, 2)
    queries = jnp.clip(jax.random.normal(key_q, (BATCH, NH, HS), jnp.float32), -4.5, 4.5)
    keys = jnp.clip(jax.random.normal(key_k, (BATCH, KVH, HS), jnp.float32), -4.5, 4.5)
    return (queries.reshape(BATCH, NH * HS), keys.reshape(BATCH, KVH * HS))


def draw_query(key, part):
    return shared_heads(key)[0].astype(jnp.bfloat16)


def draw_key_new(key, part):
    return shared_heads(key)[1].astype(jnp.bfloat16)


def draw_lengths(key, part):
    key_len, key_full = jax.random.split(jax.random.fold_in(key, 5))
    filled = jax.random.randint(key_len, (BATCH,), 1, CTX + 1)
    chosen = jax.random.randint(key_full, (), 0, BATCH)
    return jnp.where(jnp.arange(BATCH) == chosen, CTX, filled).astype(jnp.int32)


def draw_route_ids(key, part):
    keys = jax.random.split(jax.random.fold_in(key, 9), 6)
    limit = 5 * BATCH // 8
    rank_a = jax.random.permutation(keys[0], BATCH)
    other_count = jax.random.randint(keys[1], (), BATCH // 4, limit + 1)
    rank_b = jax.random.permutation(keys[2], BATCH)
    in_a = rank_a < limit
    in_b = rank_b < other_count
    flip = jax.random.randint(keys[3], (), 0, 2)
    in_zero = jnp.where(flip == 0, in_a, in_b)
    in_one = jnp.where(flip == 0, in_b, in_a)
    spare = 2 + jax.random.randint(keys[4], (BATCH,), 0, 2)
    first = jnp.where(in_zero, 0, jnp.where(in_one, 1, 2))
    second = jnp.where(in_zero & in_one, 1, jnp.where(in_zero | in_one, spare, 3))
    order = jax.random.randint(keys[5], (BATCH,), 0, 2) == 1
    left = jnp.where(order, second, first)
    right = jnp.where(order, first, second)
    return jnp.stack([left, right], axis=-1).astype(jnp.int32)


def shard_levels(key, extent, pieces, smallest, largest):
    def one(dim, shards_of):
        steps = jax.random.uniform(jax.random.fold_in(jax.random.fold_in(key, 6), dim), (shards_of,), jnp.float32, smallest / len(pieces), largest / len(pieces))
        return jnp.repeat(jnp.exp(steps), extent[dim] // shards_of).reshape((-1,) + (1,) * (len(extent) - dim - 1))

    gain = one(*pieces[0])
    for cut in pieces[1:]:
        gain = gain * one(*cut)
    return gain


def noise(rng, dims, scale, reach, cuts=(), kind=jnp.bfloat16):
    array = scale * jax.random.normal(rng, dims, jnp.float32)
    if cuts:
        array = array * shard_levels(rng, dims, cuts, -0.22, 0.18)
    return jnp.clip(array, -reach, reach).astype(kind)


def setup_inputs(seed: int = 0, part: int = 0) -> dict:
    arg_keys = jax.random.split(jax.random.key(seed), 15)
    part_splits = jax.random.split(jax.random.fold_in(arg_keys[14], part), 15)
    return {
        "stream_in": noise(part_splits[0], (BATCH, D), 1.0, 6.0, ((0, 128),)),
        "query": draw_query(jax.random.fold_in(jax.random.fold_in(arg_keys[14], part), 71), part),
        "key_new": draw_key_new(jax.random.fold_in(jax.random.fold_in(arg_keys[14], part), 71), part),
        "value_new": noise(part_splits[3], (BATCH, KVH * HS), 1.0, 6.0, ((0, 128),)),
        "key_cache": noise(part_splits[4], (BATCH, CTX, KVH * HS), 1.0, 6.0, ((0, 128),)),
        "value_cache": noise(part_splits[5], (BATCH, CTX, KVH * HS), 1.0, 6.0, ((0, 128),)),
        "lengths": draw_lengths(jax.random.fold_in(jax.random.fold_in(arg_keys[14], part), 71), part),
        "route_ids": draw_route_ids(jax.random.fold_in(jax.random.fold_in(arg_keys[14], part), 71), part),
        "route_scores": noise(part_splits[8], (BATCH, 2), 1.0, 6.0, ((0, 128),), jnp.float32),
        "out_weight": noise(arg_keys[9], (NH * HS, D), (NH * HS) ** -0.5, 0.0625, ((1, 128),)),
        "norm_gain": jnp.clip(1.0 + 0.18 * jax.random.normal(arg_keys[10], (D,), jnp.float32), 0.1, 1.9),
        "gate_weight": noise(arg_keys[11], (RESIDENT, HSPLIT * D, H // HSPLIT), D ** -0.5, 0.0625, ((1, 128),)),
        "up_weight": noise(arg_keys[12], (RESIDENT, HSPLIT * D, H // HSPLIT), D ** -0.5, 0.0625, ((1, 128),)),
        "down_weight": noise(arg_keys[13], (RESIDENT, MSPLIT * H, D // MSPLIT), H ** -0.5, 0.046875, ((1, 128),)),
    }


def attend_one(items):
    query_row, key_row, value_row, key_slots, value_slots, length = items
    group = NH // KVH
    scale = HS ** (-0.5)
    q_four = query_row.astype(jnp.float32).reshape(KVH, group, HS)
    k_own = key_row.astype(jnp.float32).reshape(KVH, HS)
    v_own = value_row.astype(jnp.float32).reshape(KVH, HS)
    k_all = key_slots.astype(jnp.float32).reshape(CTX, KVH, HS)
    v_all = value_slots.astype(jnp.float32).reshape(CTX, KVH, HS)
    scores = jnp.einsum('kgd,ckd->kgc', q_four, k_all) * scale
    live = jnp.arange(CTX, dtype=jnp.int32) < length
    scores = jnp.where(live[None, None, :], scores, -1e+30)
    own = jnp.einsum('kgd,kd->kg', q_four, k_own) * scale
    top = jnp.maximum(lax.optimization_barrier(jnp.max(scores, axis=-1)), own)
    e_cache = jnp.exp(scores - top[:, :, None])
    e_own = jnp.exp(own - top)
    total = lax.optimization_barrier(jnp.sum(e_cache, axis=-1)) + e_own
    p_cache = (e_cache / total[:, :, None]).astype(jnp.bfloat16)
    p_own = (e_own / total).astype(jnp.bfloat16)
    mixed = jnp.einsum('kgc,ckd->kgd', p_cache.astype(jnp.float32), v_all)
    mixed = mixed + p_own.astype(jnp.float32)[:, :, None] * v_own[:, None, :]
    return mixed.reshape(NH * HS).astype(jnp.bfloat16)

def reference(stream_in, query, key_new, value_new, key_cache, value_cache, lengths, route_ids, route_scores, out_weight, norm_gain, gate_weight, up_weight, down_weight):
    gate_full = gate_weight.reshape(RESIDENT, MSPLIT, HSPLIT, D // MSPLIT, H // HSPLIT).transpose(0, 1, 3, 2, 4).reshape(RESIDENT, D, H)
    up_full = up_weight.reshape(RESIDENT, MSPLIT, HSPLIT, D // MSPLIT, H // HSPLIT).transpose(0, 1, 3, 2, 4).reshape(RESIDENT, D, H)
    down_full = down_weight.reshape(RESIDENT, MSPLIT, HSPLIT, H // HSPLIT, D // MSPLIT).transpose(0, 2, 3, 1, 4).reshape(RESIDENT, H, D)
    attn = lax.map(attend_one, (query, key_new, value_new, key_cache, value_cache, lengths))
    proj = jnp.dot(attn, out_weight, preferred_element_type=jnp.float32).astype(jnp.bfloat16)
    resid = stream_in.astype(jnp.float32) + proj.astype(jnp.float32)
    power = lax.optimization_barrier(jnp.mean(resid * resid, axis=-1, keepdims=True))
    normed = (resid * lax.rsqrt(power + 1e-05) * norm_gain).astype(jnp.bfloat16)
    probs = jax.nn.softmax(route_scores, axis=-1)
    columns = []
    for expert in range(RESIDENT):
        columns.append(lax.optimization_barrier(jnp.sum(jnp.where(route_ids == expert, probs, 0.0), axis=-1)))
    weight = jnp.stack(columns, axis=-1).astype(jnp.bfloat16)
    ffn = jnp.zeros(resid.shape, jnp.float32)
    for expert in range(RESIDENT):
        gate = jnp.dot(normed, gate_full[expert], preferred_element_type=jnp.float32)
        upper = jnp.dot(normed, up_full[expert], preferred_element_type=jnp.float32)
        hidden = (jax.nn.silu(gate) * upper).astype(jnp.bfloat16)
        result = jnp.dot(hidden, down_full[expert], preferred_element_type=jnp.float32)
        ffn = ffn + weight[:, expert].astype(jnp.float32)[:, None] * result
    return (resid + ffn).astype(jnp.bfloat16)
```

```python
import functools

import jax
import jax.numpy as jnp
from jax import lax
from jax.experimental import pallas as pl
from jax.experimental.pallas import tpu as pltpu
from jax.sharding import PartitionSpec as P

NH = 64
KVH = 8
HS = 128
RESIDENT = 2
MSPLIT = 8
PLANE = 8
LANES = 128
BF16 = jnp.bfloat16
F32 = jnp.float32
MESH = pl.DeviceIdType.MESH


def nt_dot(a, b):
    return lax.dot_general(a, b, (((1,), (1,)), ((), ())), preferred_element_type=F32)


def nn_dot(a, b):
    return lax.dot_general(a, b, (((1,), (0,)), ((), ())), preferred_element_type=F32)


def copy_to(src, dst, send, recv, target):
    return pltpu.make_async_remote_copy(
        src_ref=src,
        dst_ref=dst,
        send_sem=send,
        recv_sem=recv,
        device_id={"gx": target},
        device_id_type=MESH,
    )


def wait_bytes(ref, sem):
    pltpu.make_async_copy(ref, ref, sem).wait()


def each(count, body, start=0):
    def step(i, carry):
        body(i)
        return carry

    lax.fori_loop(start, count, step, 0)


def layer_kernel(
    cfg,
    lengths,
    route_ids,
    route_scores,
    stream_in,
    query,
    key_new,
    value_new,
    gain,
    key_cache,
    value_cache,
    out_weight,
    gate_weight,
    up_weight,
    down_weight,
    out_ref,
    kbuf,
    vbuf,
    gbuf,
    ubuf,
    dwbuf,
    wbuf,
    qf,
    sf,
    sblk,
    att,
    abuf,
    af,
    pbuf,
    dbuf,
    sbuf,
    meta_out,
    meta_in,
    meta_blk,
    meta_all,
    resid_ref,
    yblk,
    xbuf,
    ssq_row,
    ssq_all,
    xcs,
    own,
    rs_send,
    rs_recv,
    hbuf,
    kout,
    kin,
    lf,
    lout,
    lbuf,
    loc_sem,
    one_send,
    one_recv,
    st_send,
    st_recv,
    me_send,
    me_recv,
    rs_sem,
    ag_sem,
    l_send,
    l_recv,
):
    n = cfg["n"]
    hsplit = n // MSPLIT
    planes = n // PLANE
    batch = n
    width = cfg["width"]
    bw = width // MSPLIT
    pieces = cfg["hidden"] // LANES
    per = cfg["per"]
    pad = cfg["pad"]
    quarters = MSPLIT // RESIDENT
    rows = quarters * pad

    me = lax.axis_index("gx")
    z = me // PLANE
    k = lax.rem(me, PLANE)
    m = me // hsplit
    h = lax.rem(me, hsplit)
    low = me - m * hsplit
    sgn = 1 - 2 * lax.rem(me, 2)

    barrier = pltpu.get_barrier_semaphore()

    def greet(i):
        pl.semaphore_signal(
            barrier, inc=1, device_id={"gx": lax.rem(me + i, n)}, device_id_type=MESH
        )

    each(n, greet, 1)

    loads = [
        pltpu.make_async_copy(key_cache, kbuf, loc_sem.at[0]),
        pltpu.make_async_copy(value_cache, vbuf, loc_sem.at[1]),
        pltpu.make_async_copy(gate_weight, gbuf, loc_sem.at[2]),
        pltpu.make_async_copy(up_weight, ubuf, loc_sem.at[3]),
        pltpu.make_async_copy(down_weight, dwbuf, loc_sem.at[4]),
        pltpu.make_async_copy(
            out_weight.at[:, pl.ds(pl.multiple_of(k * bw, bw), bw)], wbuf.at[k], loc_sem.at[5]
        ),
    ]
    for load in loads:
        load.start()

    for j in range(width // LANES):
        cols = slice(j * LANES, (j + 1) * LANES)
        qf[j : j + 1, :] = query[0:1, cols].astype(F32)
        sf[j : j + 1, :] = stream_in[0:1, cols].astype(F32)
    sblk[...] = sf[...].reshape(MSPLIT, 8, LANES).astype(BF16)

    lane = lax.broadcasted_iota(jnp.int32, (1, LANES), 1)
    s0 = jnp.full((1, LANES), route_scores[0, 0], F32)
    s1 = jnp.full((1, LANES), route_scores[0, 1], F32)
    top = jnp.maximum(s0, s1)
    e0 = jnp.exp(s0 - top)
    e1 = jnp.exp(s1 - top)
    q0 = e0 / (e0 + e1)
    q1 = e1 / (e0 + e1)
    id0 = jnp.full((1, LANES), route_ids[0, 0], jnp.int32)
    id1 = jnp.full((1, LANES), route_ids[0, 1], jnp.int32)
    meta = jnp.zeros((1, LANES), F32)
    for e in range(RESIDENT):
        w = jnp.where(id0 == e, q0, 0.0) + jnp.where(id1 == e, q1, 0.0)
        w = w.astype(BF16).astype(F32)
        picked = jnp.where((id0 == e) | (id1 == e), 1.0, 0.0)
        meta = jnp.where(lane == e, w, meta)
        meta = jnp.where(lane == RESIDENT + e, picked, meta)
    meta_out[...] = meta

    loads[0].wait()
    loads[1].wait()
    scale = HS ** (-0.5)
    slots = kbuf.shape[0]
    live = lax.broadcasted_iota(jnp.int32, (NH // KVH, slots), 1) < lengths[0]
    for g in range(KVH):
        cols = slice(g * HS, (g + 1) * HS)
        q_g = qf[g * 8 : (g + 1) * 8, :]
        k_own = key_new[0:1, cols].astype(F32)
        v_own = value_new[0:1, cols].astype(F32)
        s = nt_dot(q_g.astype(BF16), kbuf[:, cols]) * scale
        s = jnp.where(live, s, -1e30)
        o = jnp.sum(q_g * k_own, axis=1, keepdims=True) * scale
        t = jnp.maximum(jnp.max(s, axis=1, keepdims=True), o)
        es = jnp.exp(s - t)
        eo = jnp.exp(o - t)
        total = jnp.sum(es, axis=1, keepdims=True) + eo
        p = (es / total).astype(BF16)
        po = (eo / total).astype(BF16).astype(F32)
        att[g] = (nn_dot(p, vbuf[:, cols]) + po * v_own).astype(BF16)

    pl.semaphore_wait(barrier, n - 1)

    def plane_send(i):
        j = lax.rem(k + i, PLANE)
        copy_to(
            att.at[j], abuf.at[z, k], one_send.at[0], one_recv.at[0], z * PLANE + j
        ).start()

    each(PLANE, plane_send, 1)

    def w_send(i):
        j = lax.rem(k + i, PLANE)
        copy_to(
            out_weight.at[:, pl.ds(pl.multiple_of(j * bw, bw), bw)],
            wbuf.at[k],
            one_send.at[1],
            one_recv.at[1],
            z * PLANE + j,
        ).start()

    each(PLANE, w_send, 1)

    def stream_send(j):
        target = j * hsplit + z

        @pl.when(target != me)
        def _():
            copy_to(sblk.at[j], sbuf.at[k], st_send.at[j], st_recv.at[k], target).start()
            copy_to(meta_out, meta_in.at[k], me_send.at[j], me_recv.at[k], target).start()

    each(MSPLIT, stream_send)

    @pl.when(z == h)
    def _():
        sbuf[k] = sblk[m]
        meta_in[k] = meta_out[...]

    abuf[z, k] = att[k]
    wait_bytes(abuf.at[0, pl.ds(0, PLANE - 1)], one_recv.at[0])

    def z_send(i):
        target = lax.rem(z + i, planes)
        copy_to(
            abuf.at[z], abuf.at[z], one_send.at[2], one_recv.at[2], target * PLANE + k
        ).start()

    each(planes, z_send, 1)

    def stream_recv(i):
        source = h * PLANE + i

        @pl.when(source != me)
        def _():
            wait_bytes(sbuf.at[i], st_recv.at[i])
            wait_bytes(meta_in.at[i], me_recv.at[i])

    each(PLANE, stream_recv)

    loads[5].wait()
    wait_bytes(wbuf.at[pl.ds(0, PLANE - 1)], one_recv.at[1])
    wait_bytes(abuf.at[pl.ds(0, planes - 1)], one_recv.at[2])

    af[...] = abuf[...].reshape(batch * 8, LANES).astype(F32)
    a = jnp.concatenate(
        [af[pl.ds(j, batch, stride=8), :] for j in range(8)], axis=1
    ).astype(BF16)
    part = nt_dot(a, wbuf[...].reshape(PLANE * wbuf.shape[1], bw))
    pbuf[...] = part.astype(BF16).reshape(hsplit, 8, part.shape[1])

    def proj_send(i):
        j = lax.rem(h + i, hsplit)
        copy_to(pbuf.at[j], dbuf.at[h], one_send.at[3], one_recv.at[3], m * hsplit + j).start()

    each(hsplit, proj_send, 1)
    dbuf[h] = pbuf[h]

    lf[...] = sbuf[...].reshape(PLANE * 8, LANES).astype(F32)
    stream = jnp.concatenate([lf[pl.ds(c, 8, stride=8), :] for c in range(8)], axis=1)
    g8 = gain[pl.ds(pl.multiple_of(m * 8, 8), 8), :]
    gain_row = jnp.concatenate([g8[c : c + 1, :] for c in range(8)], axis=1)
    route = jnp.concatenate([meta_in[i] for i in range(PLANE)], axis=0)

    wait_bytes(dbuf.at[pl.ds(0, hsplit - 1)], one_recv.at[3])
    halves = []
    for half in range(hsplit // PLANE):
        acc = dbuf[half * PLANE].astype(F32)
        for j in range(1, PLANE):
            acc = acc + dbuf[half * PLANE + j].astype(F32)
        halves.append(acc)
    proj = jnp.concatenate(halves, axis=1).astype(BF16).astype(F32)
    resid = stream + proj
    resid_ref[...] = resid
    ssq = jnp.sum(resid * resid, axis=1, keepdims=True)
    lane8 = lax.broadcasted_iota(jnp.int32, (8, LANES), 1)
    meta_blk[...] = jnp.where(lane8 == 2 * RESIDENT, ssq, route)
    meta_all[h] = meta_blk[...]
    yblk[...] = (resid * gain_row).astype(BF16)
    xbuf[h] = yblk[...]

    def spread(i):
        target = m * hsplit + lax.rem(h + i, hsplit)
        copy_to(meta_blk, meta_all.at[h], one_send.at[4], one_recv.at[4], target).start()
        copy_to(yblk, xbuf.at[h], one_send.at[5], one_recv.at[5], target).start()

    each(hsplit, spread, 1)
    wait_bytes(meta_all.at[pl.ds(0, hsplit - 1)], one_recv.at[4])

    info = meta_all[...].reshape(batch, LANES)
    info_t = info.T
    ia = lax.broadcasted_iota(jnp.int32, (batch, batch), 0)
    ib = lax.broadcasted_iota(jnp.int32, (batch, batch), 1)
    before_t = jnp.where(ia < ib, 1.0, 0.0).astype(BF16)
    before = jnp.where(ib < ia, 1.0, 0.0).astype(BF16)
    ranks_t = nn_dot(info_t[0:8].astype(BF16), before_t)
    ranks = nn_dot(before, info.astype(BF16))

    def place_of(rank, picked):
        out = rank
        for c in range(1, quarters):
            out = out + jnp.where(rank >= float(c * per), float(pad - per), 0.0)
        return jnp.where(picked > 0.5, out, -1.0)

    rows_i = [place_of(ranks_t[RESIDENT + e : RESIDENT + e + 1], info_t[RESIDENT + e : RESIDENT + e + 1]) for e in range(RESIDENT)]
    cols_i = [place_of(ranks[:, RESIDENT + e : RESIDENT + e + 1], info[:, RESIDENT + e : RESIDENT + e + 1]) for e in range(RESIDENT)]
    ssq_row[...] = info_t[2 * RESIDENT : 2 * RESIDENT + 1]
    ssq_all[m] = ssq_row[...]

    def ssq_send(i):
        j = lax.rem(m + i, MSPLIT)
        copy_to(ssq_row, ssq_all.at[m], one_send.at[6], one_recv.at[6], j * hsplit + low).start()

    each(MSPLIT, ssq_send, 1)

    wait_bytes(xbuf.at[pl.ds(0, hsplit - 1)], one_recv.at[5])
    x = xbuf[...].reshape(batch, bw)
    r_iota = lax.broadcasted_iota(jnp.int32, (rows, batch), 0).astype(F32)
    for e in range(RESIDENT):
        pick = jnp.where(r_iota == rows_i[e], 1.0, 0.0).astype(BF16)
        xcs[e] = nn_dot(pick, x).astype(BF16)
    loads[2].wait()
    loads[3].wait()

    fwd = MSPLIT // 2
    bwd = MSPLIT - 1 - fwd

    def ring(step):
        return lax.rem(m + sgn * step + 2 * MSPLIT, MSPLIT)

    next_dev = ring(1) * hsplit + low
    prev_dev = ring(-1) * hsplit + low

    def rs_copy(slot, q, target):
        return copy_to(
            rs_send.at[slot, q], rs_recv.at[slot, q], one_send.at[7], rs_sem.at[slot, q], target
        )

    def first(q):
        cols = pl.ds(pl.multiple_of(q * LANES, LANES), LANES)
        for e in range(RESIDENT):
            rhs = jnp.concatenate([gbuf[e, :, cols], ubuf[e, :, cols]], axis=1)
            r = nn_dot(xcs[e], rhs)
            own[q, e * quarters : (e + 1) * quarters] = r.reshape(quarters, pad, 2 * LANES)
        rs_send[0, q] = own[q, ring(fwd)].astype(BF16)
        rs_copy(0, q, next_dev).start()
        rs_send[fwd, q] = own[q, ring(-bwd)].astype(BF16)
        rs_copy(fwd, q, prev_dev).start()

    each(pieces, first)

    for t in range(1, fwd):

        def onward(q, t=t):
            wait_bytes(rs_recv.at[t - 1, q], rs_sem.at[t - 1, q])
            v = rs_recv[t - 1, q].astype(F32) + own[q, ring(fwd - t)]
            rs_send[t, q] = v.astype(BF16)
            rs_copy(t, q, next_dev).start()
            if t < bwd:
                b = fwd + t
                wait_bytes(rs_recv.at[b - 1, q], rs_sem.at[b - 1, q])
                v = rs_recv[b - 1, q].astype(F32) + own[q, ring(t - bwd)]
                rs_send[b, q] = v.astype(BF16)
                rs_copy(b, q, prev_dev).start()

        each(pieces, onward)

    wait_bytes(ssq_all.at[pl.ds(0, MSPLIT - 1)], one_recv.at[6])
    power = ssq_all[0]
    for j in range(1, MSPLIT):
        power = power + ssq_all[j]
    chunk_row = jnp.where(m < quarters, rows_i[0], rows_i[1])
    c_iota = lax.broadcasted_iota(jnp.int32, (pad, batch), 0) + lax.rem(m, quarters) * pad
    hit = c_iota.astype(F32) == chunk_row
    mean = jnp.sum(jnp.where(hit, power, 0.0), axis=1, keepdims=True) / float(width)
    factor = lax.rsqrt(mean + 1e-05)

    def ag_copy(slot, q, chunk, target):
        return copy_to(
            hbuf.at[q, chunk], hbuf.at[q, chunk], one_send.at[8], ag_sem.at[slot, q], target
        )

    def finish(q):
        wait_bytes(rs_recv.at[fwd - 1, q], rs_sem.at[fwd - 1, q])
        wait_bytes(rs_recv.at[MSPLIT - 2, q], rs_sem.at[MSPLIT - 2, q])
        v = own[q, m] + rs_recv[fwd - 1, q].astype(F32) + rs_recv[MSPLIT - 2, q].astype(F32)
        v = v * factor
        ga = v[:, :LANES]
        up = v[:, LANES:]
        hbuf[q, m] = (ga / (1.0 + jnp.exp(-ga)) * up).astype(BF16)
        ag_copy(0, q, m, next_dev).start()
        ag_copy(fwd, q, m, prev_dev).start()

    each(pieces, finish)

    for t in range(1, fwd):

        def relay(q, t=t):
            wait_bytes(hbuf.at[q, ring(-t)], ag_sem.at[t - 1, q])
            ag_copy(t, q, ring(-t), next_dev).start()
            if t < bwd:
                b = fwd + t
                wait_bytes(hbuf.at[q, ring(t)], ag_sem.at[b - 1, q])
                ag_copy(b, q, ring(t), prev_dev).start()

        each(pieces, relay)

    def arrived(q):
        wait_bytes(hbuf.at[q, ring(-fwd)], ag_sem.at[fwd - 1, q])
        wait_bytes(hbuf.at[q, ring(bwd)], ag_sem.at[MSPLIT - 2, q])

    each(pieces, arrived)

    loads[4].wait()
    col_iota = lax.broadcasted_iota(jnp.int32, (batch, rows), 1).astype(F32)
    spreads = []
    for e in range(RESIDENT):
        hc = jnp.concatenate(
            [hbuf[q, e * quarters : (e + 1) * quarters].reshape(rows, LANES) for q in range(pieces)],
            axis=1,
        )
        pick = jnp.where(col_iota == cols_i[e], 1.0, 0.0).astype(BF16)
        spreads.append(nn_dot(pick, hc).astype(BF16))
    tile = 256
    for c in range(bw // tile):
        cols = slice(c * tile, (c + 1) * tile)
        total = jnp.zeros((batch, tile), F32)
        for e in range(RESIDENT):
            total = total + info[:, e : e + 1] * nn_dot(spreads[e], dwbuf[e, :, cols])
        kout[:, :, cols] = total.astype(BF16).reshape(hsplit, 8, tile)

    def ffn_send(i):
        j = lax.rem(h + i, hsplit)
        copy_to(kout.at[j], kin.at[h], one_send.at[9], one_recv.at[7], m * hsplit + j).start()

    each(hsplit, ffn_send, 1)
    kin[h] = kout[h]
    wait_bytes(kin.at[pl.ds(0, hsplit - 1)], one_recv.at[7])
    ffn = kin[0].astype(F32)
    for j in range(1, hsplit):
        ffn = ffn + kin[j].astype(F32)
    final = resid_ref[...] + ffn
    for c in range(8):
        lf[pl.ds(c, 8, stride=8), :] = final[:, c * LANES : (c + 1) * LANES]
    lout[...] = lf[...].reshape(PLANE, 8, LANES).astype(BF16)

    def row_send(i):
        target = h * PLANE + i

        @pl.when(target != me)
        def _():
            copy_to(lout.at[i], lbuf.at[m], l_send.at[i], l_recv.at[m], target).start()

    each(PLANE, row_send)

    @pl.when(z == h)
    def _():
        lbuf[m] = lout[k]

    wait_bytes(abuf.at[0, pl.ds(0, PLANE - 1)], one_send.at[0])
    wait_bytes(wbuf.at[pl.ds(0, PLANE - 1)], one_send.at[1])
    wait_bytes(abuf.at[pl.ds(0, planes - 1)], one_send.at[2])
    wait_bytes(dbuf.at[pl.ds(0, hsplit - 1)], one_send.at[3])
    wait_bytes(meta_all.at[pl.ds(0, hsplit - 1)], one_send.at[4])
    wait_bytes(xbuf.at[pl.ds(0, hsplit - 1)], one_send.at[5])
    wait_bytes(ssq_all.at[pl.ds(0, MSPLIT - 1)], one_send.at[6])
    wait_bytes(rs_send, one_send.at[7])
    wait_bytes(hbuf.at[:, pl.ds(0, MSPLIT - 1)], one_send.at[8])
    wait_bytes(kin.at[pl.ds(0, hsplit - 1)], one_send.at[9])

    def drain(j):
        @pl.when(j * hsplit + z != me)
        def _():
            wait_bytes(sblk.at[j], st_send.at[j])
            wait_bytes(meta_out, me_send.at[j])
            wait_bytes(lbuf.at[j], l_recv.at[j])

        @pl.when(h * PLANE + j != me)
        def _():
            wait_bytes(lout.at[j], l_send.at[j])

    each(MSPLIT, drain)

    qf[...] = lbuf[...].reshape(MSPLIT * 8, LANES).astype(F32)
    for j in range(width // LANES):
        out_ref[0:1, j * LANES : (j + 1) * LANES] = qf[j : j + 1, :].astype(BF16)


def on_device(
    stream_in,
    query,
    key_new,
    value_new,
    key_cache,
    value_cache,
    lengths,
    route_ids,
    route_scores,
    out_weight,
    norm_gain,
    gate_weight,
    up_weight,
    down_weight,
):
    n = lax.axis_size("gx")
    width = stream_in.shape[1]
    slots = key_cache.shape[1]
    kv = key_cache.shape[2]
    hidden = gate_weight.shape[2]
    bw = width // MSPLIT
    hsplit = n // MSPLIT
    planes = n // PLANE
    cols = out_weight.shape[1]
    quarters = MSPLIT // RESIDENT
    per = -(-(5 * n // 8) // quarters)
    pad = -(-per // 8) * 8
    pieces = hidden // LANES
    cfg = dict(n=n, width=width, hidden=hidden, per=per, pad=pad)
    hops = MSPLIT - 1

    def vmem(*shape, dtype=BF16):
        return pltpu.VMEM(shape, dtype)

    scratch = [
        vmem(slots, kv),
        vmem(slots, kv),
        vmem(*gate_weight.shape),
        vmem(*up_weight.shape),
        vmem(*down_weight.shape),
        vmem(PLANE, cols, bw),
        vmem(width // LANES, LANES, dtype=F32),
        vmem(width // LANES, LANES, dtype=F32),
        vmem(MSPLIT, 8, LANES),
        vmem(KVH, 8, HS),
        vmem(planes, PLANE, 8, HS),
        vmem(n * 8, LANES, dtype=F32),
        vmem(hsplit, 8, PLANE * cols),
        vmem(hsplit, 8, PLANE * cols),
        vmem(PLANE, 8, LANES),
        vmem(1, LANES, dtype=F32),
        vmem(PLANE, 1, LANES, dtype=F32),
        vmem(8, LANES, dtype=F32),
        vmem(hsplit, 8, LANES, dtype=F32),
        vmem(8, bw, dtype=F32),
        vmem(8, bw),
        vmem(hsplit, 8, bw),
        vmem(1, LANES, dtype=F32),
        vmem(MSPLIT, 1, LANES, dtype=F32),
        vmem(RESIDENT, quarters * pad, bw),
        vmem(pieces, MSPLIT, pad, 2 * LANES, dtype=F32),
        vmem(hops, pieces, pad, 2 * LANES),
        vmem(hops, pieces, pad, 2 * LANES),
        vmem(pieces, MSPLIT, pad, LANES),
        vmem(hsplit, 8, bw),
        vmem(hsplit, 8, bw),
        vmem(PLANE * 8, LANES, dtype=F32),
        vmem(PLANE, 8, LANES),
        vmem(MSPLIT, 8, LANES),
        pltpu.SemaphoreType.DMA((6,)),
        pltpu.SemaphoreType.DMA((10,)),
        pltpu.SemaphoreType.DMA((8,)),
        pltpu.SemaphoreType.DMA((MSPLIT,)),
        pltpu.SemaphoreType.DMA((PLANE,)),
        pltpu.SemaphoreType.DMA((MSPLIT,)),
        pltpu.SemaphoreType.DMA((PLANE,)),
        pltpu.SemaphoreType.DMA((hops, pieces)),
        pltpu.SemaphoreType.DMA((hops, pieces)),
        pltpu.SemaphoreType.DMA((PLANE,)),
        pltpu.SemaphoreType.DMA((MSPLIT,)),
    ]
    smem = pl.BlockSpec(memory_space=pltpu.SMEM)
    local = pl.BlockSpec(memory_space=pltpu.VMEM)
    anywhere = pl.BlockSpec(memory_space=pl.ANY)
    return pl.pallas_call(
        functools.partial(layer_kernel, cfg),
        out_shape=jax.ShapeDtypeStruct((1, width), BF16),
        in_specs=[smem] * 3 + [local] * 5 + [anywhere] * 6,
        out_specs=local,
        scratch_shapes=scratch,
        compiler_params=pltpu.CompilerParams(
            collective_id=0, has_side_effects=True, vmem_limit_bytes=60 * 1024 * 1024
        ),
        name="layer",
    )(
        lengths,
        route_ids,
        route_scores,
        stream_in,
        query,
        key_new,
        value_new,
        norm_gain.reshape(width // LANES, LANES),
        key_cache.reshape(slots, kv),
        value_cache.reshape(slots, kv),
        out_weight.T,
        gate_weight,
        up_weight,
        down_weight,
    )


def solution(mesh):
    rows = P(("groups", "gx"), None)
    in_specs = (
        rows,
        rows,
        rows,
        rows,
        P(("groups", "gx"), None, None),
        P(("groups", "gx"), None, None),
        P(("groups", "gx")),
        rows,
        rows,
        P(None, "gx"),
        P(),
        P(None, "gx", None),
        P(None, "gx", None),
        P(None, "gx", None),
    )
    return jax.shard_map(
        on_device, mesh=mesh, in_specs=in_specs, out_specs=rows, check_vma=False
    )
```

```python
import functools

import jax
import jax.numpy as jnp
from jax import lax
from jax.experimental import pallas as pl
from jax.experimental.pallas import tpu as pltpu
from jax.sharding import PartitionSpec as P

NH = 64
KVH = 8
HS = 128
RESIDENT = 2
MSPLIT = 8
PLANE = 8
LANES = 128
BF16 = jnp.bfloat16
F32 = jnp.float32
MESH = pl.DeviceIdType.MESH


def nt_dot(a, b):
    return lax.dot_general(a, b, (((1,), (1,)), ((), ())), preferred_element_type=F32)


def nn_dot(a, b):
    return lax.dot_general(a, b, (((1,), (0,)), ((), ())), preferred_element_type=F32)


def copy_to(src, dst, send, recv, target):
    return pltpu.make_async_remote_copy(
        src_ref=src,
        dst_ref=dst,
        send_sem=send,
        recv_sem=recv,
        device_id={"gx": target},
        device_id_type=MESH,
    )


def wait_bytes(ref, sem):
    pltpu.make_async_copy(ref, ref, sem).wait()


def each(count, body, start=0):
    def step(i, carry):
        body(i)
        return carry

    lax.fori_loop(start, count, step, 0)


def layer_kernel(
    cfg,
    lengths,
    route_ids,
    route_scores,
    stream_in,
    query,
    key_new,
    value_new,
    gain,
    key_cache,
    value_cache,
    out_weight,
    gate_weight,
    up_weight,
    down_weight,
    out_ref,
    kbuf,
    vbuf,
    gbuf,
    ubuf,
    dwbuf,
    wbuf,
    qf,
    sf,
    sblk,
    att,
    abuf,
    af,
    pbuf,
    dbuf,
    sbuf,
    meta_out,
    meta_in,
    meta_blk,
    meta_all,
    resid_ref,
    yblk,
    xbuf,
    ssq_row,
    ssq_all,
    xcs,
    own,
    rs_send,
    rs_recv,
    hbuf,
    kout,
    kin,
    lf,
    lout,
    lbuf,
    svm,
    qvm,
    knvm,
    vnvm,
    gainvm,
    loc_sem,
    one_send,
    one_recv,
    z_recv,
    tok,
    size_send,
    st_send,
    st_recv,
    me_send,
    me_recv,
    rs_sem,
    ag_sem,
    l_send,
    l_recv,
):
    n = cfg["n"]
    hsplit = n // MSPLIT
    planes = n // PLANE
    batch = n
    width = cfg["width"]
    bw = width // MSPLIT
    pieces = cfg["hidden"] // LANES
    edges = cfg["edges"]
    pad = cfg["pad"]
    short = cfg["short"]
    quarters = MSPLIT // RESIDENT
    rows = quarters * pad
    hops = MSPLIT - 1

    me = lax.axis_index("gx")
    z = me // PLANE
    k = lax.rem(me, PLANE)
    m = me // hsplit
    h = lax.rem(me, hsplit)
    low = me - m * hsplit
    sgn = 1 - 2 * lax.rem(me, 2)

    def up(step):
        return lax.rem(z + sgn * step + 2 * planes, planes)

    def signal(sem, target):
        pl.semaphore_signal(sem, inc=1, device_id={"gx": target}, device_id_type=MESH)

    small = [
        pltpu.make_async_copy(src, dst, loc_sem.at[6 + i])
        for i, (src, dst) in enumerate(
            [(query, qvm), (key_new, knvm), (value_new, vnvm), (stream_in, svm), (gain, gainvm)]
        )
    ]
    for load in small:
        load.start()
    loads = [
        pltpu.make_async_copy(key_cache, kbuf, loc_sem.at[0]),
        pltpu.make_async_copy(value_cache, vbuf, loc_sem.at[1]),
        pltpu.make_async_copy(gate_weight, gbuf, loc_sem.at[2]),
        pltpu.make_async_copy(up_weight, ubuf, loc_sem.at[3]),
        pltpu.make_async_copy(down_weight, dwbuf, loc_sem.at[4]),
        pltpu.make_async_copy(
            out_weight.at[:, pl.ds(pl.multiple_of(k * bw, bw), bw)], wbuf.at[k], loc_sem.at[5]
        ),
    ]
    for load in loads[:2]:
        load.start()

    barrier = pltpu.get_barrier_semaphore()

    for step in (1, -1):
        signal(barrier, up(step) * PLANE + k)

    def greet(i):
        signal(barrier, z * PLANE + lax.rem(k + i, PLANE))

    each(PLANE, greet, 1)

    for load in loads[2:]:
        load.start()

    lane = lax.broadcasted_iota(jnp.int32, (1, LANES), 1)
    s0 = jnp.full((1, LANES), route_scores[0, 0], F32)
    s1 = jnp.full((1, LANES), route_scores[0, 1], F32)
    top = jnp.maximum(s0, s1)
    e0 = jnp.exp(s0 - top)
    e1 = jnp.exp(s1 - top)
    q0 = e0 / (e0 + e1)
    q1 = e1 / (e0 + e1)
    id0 = jnp.full((1, LANES), route_ids[0, 0], jnp.int32)
    id1 = jnp.full((1, LANES), route_ids[0, 1], jnp.int32)
    meta = jnp.zeros((1, LANES), F32)
    for e in range(RESIDENT):
        w = jnp.where(id0 == e, q0, 0.0) + jnp.where(id1 == e, q1, 0.0)
        w = w.astype(BF16).astype(F32)
        picked = jnp.where((id0 == e) | (id1 == e), 1.0, 0.0)
        meta = jnp.where(lane == e, w, meta)
        meta = jnp.where(lane == RESIDENT + e, picked, meta)
    meta_out[...] = meta

    for load in small[:3]:
        load.wait()
    for j in range(width // LANES):
        qf[j : j + 1, :] = qvm[0:1, j * LANES : (j + 1) * LANES].astype(F32)

    def per_group(row_ref):
        return jnp.concatenate(
            [
                jnp.broadcast_to(row_ref[0:1, g * HS : (g + 1) * HS].astype(F32), (NH // KVH, HS))
                for g in range(KVH)
            ],
            axis=0,
        )

    q_all = qf[...]
    scale = HS ** (-0.5)
    o = jnp.sum(q_all * per_group(knvm), axis=1, keepdims=True) * scale
    v_own = per_group(vnvm)
    loads[0].wait()
    slots = kbuf.shape[0]
    s = jnp.concatenate(
        [
            nt_dot(q_all[g * 8 : (g + 1) * 8].astype(BF16), kbuf[:, g * HS : (g + 1) * HS])
            for g in range(KVH)
        ],
        axis=0,
    )
    live = lax.broadcasted_iota(jnp.int32, (NH, slots), 1) < lengths[0]
    s = jnp.where(live, s * scale, -1e30)
    t = jnp.maximum(jnp.max(s, axis=1, keepdims=True), o)
    es = jnp.exp(s - t)
    eo = jnp.exp(o - t)
    total = jnp.sum(es, axis=1, keepdims=True) + eo
    p = es / total
    own_term = (eo / total).astype(BF16).astype(F32) * v_own
    loads[1].wait()
    for g in range(KVH):
        r = slice(g * 8, (g + 1) * 8)
        mixed = nn_dot(p[r].astype(BF16), vbuf[:, g * HS : (g + 1) * HS])
        att[g] = (mixed + own_term[r]).astype(BF16)

    pl.semaphore_wait(barrier, PLANE + 1)
    for step in (1, -1):
        signal(tok.at[0], up(step) * PLANE + k)

    def plane_send(i):
        j = lax.rem(k + i, PLANE)
        copy_to(
            att.at[j], abuf.at[z, k], one_send.at[0], one_recv.at[0], z * PLANE + j
        ).start()

    each(PLANE, plane_send, 1)

    def w_send(i):
        j = lax.rem(k + i, PLANE)
        copy_to(
            out_weight.at[:, pl.ds(pl.multiple_of(j * bw, bw), bw)],
            wbuf.at[k],
            one_send.at[1],
            one_recv.at[1],
            z * PLANE + j,
        ).start()

    each(PLANE, w_send, 1)

    abuf[z, k] = att[k]
    pl.semaphore_wait(tok.at[0], 2)
    for step in (2, -2):
        signal(tok.at[1], up(step) * PLANE + k)
    wait_bytes(abuf.at[0, pl.ds(0, PLANE - 1)], one_recv.at[0])
    pl.semaphore_wait(tok.at[1], 2)

    def z_copy(origin, step):
        return copy_to(
            abuf.at[origin],
            abuf.at[origin],
            one_send.at[2],
            z_recv.at[origin],
            up(step) * PLANE + k,
        )

    reach = planes // 4
    for step in range(reach, 0, -1):
        z_copy(z, step).start()
        z_copy(z, -step).start()
    for step in (reach, -reach):
        signal(tok.at[2], up(step) * PLANE + k)
    for load in small[3:]:
        load.wait()
    for j in range(width // LANES):
        sf[j : j + 1, :] = svm[0:1, j * LANES : (j + 1) * LANES].astype(F32)
    sblk[...] = sf[...].reshape(MSPLIT, 8, LANES).astype(BF16)
    far = up(-reach)
    wait_bytes(abuf.at[far], z_recv.at[far])
    for step in range(reach, 0, -1):
        z_copy(far, step).start()
    near = up(reach)
    wait_bytes(abuf.at[near], z_recv.at[near])
    for step in range(reach - 1, 0, -1):
        z_copy(near, -step).start()
    pl.semaphore_wait(tok.at[2], 2)
    for step in (1, -1):
        signal(tok.at[3], up(step) * PLANE + k)
    pl.semaphore_wait(tok.at[3], 2)

    def stream_send(j):
        target = j * hsplit + z

        @pl.when(target != me)
        def _():
            copy_to(sblk.at[j], sbuf.at[k], st_send.at[j], st_recv.at[k], target).start()
            copy_to(meta_out, meta_in.at[k], me_send.at[j], me_recv.at[k], target).start()

    each(MSPLIT, stream_send)

    @pl.when(z == h)
    def _():
        sbuf[k] = sblk[m]
        meta_in[k] = meta_out[...]

    def z_wait(i):
        origin = lax.rem(z + i, planes)

        @pl.when((origin != far) & (origin != near))
        def _():
            wait_bytes(abuf.at[origin], z_recv.at[origin])

    each(planes, z_wait, 1)

    loads[5].wait()
    wait_bytes(wbuf.at[pl.ds(0, PLANE - 1)], one_recv.at[1])

    af[...] = abuf[...].reshape(batch * 8, LANES).astype(F32)
    a = jnp.concatenate(
        [af[pl.ds(j, batch, stride=8), :] for j in range(8)], axis=1
    ).astype(BF16)
    part = nt_dot(a, wbuf[...].reshape(PLANE * wbuf.shape[1], bw))
    pbuf[...] = part.astype(BF16).reshape(hsplit, 8, part.shape[1])

    def proj_send(i):
        j = lax.rem(h + i, hsplit)
        copy_to(pbuf.at[j], dbuf.at[h], one_send.at[3], one_recv.at[3], m * hsplit + j).start()

    each(hsplit, proj_send, 1)
    dbuf[h] = pbuf[h]

    def stream_recv(i):
        source = h * PLANE + i

        @pl.when(source != me)
        def _():
            wait_bytes(sbuf.at[i], st_recv.at[i])
            wait_bytes(meta_in.at[i], me_recv.at[i])

    each(PLANE, stream_recv)

    lf[...] = sbuf[...].reshape(PLANE * 8, LANES).astype(F32)
    stream = jnp.concatenate([lf[pl.ds(c, 8, stride=8), :] for c in range(8)], axis=1)
    g8 = gainvm[pl.ds(pl.multiple_of(m * 8, 8), 8), :]
    gain_row = jnp.concatenate([g8[c : c + 1, :] for c in range(8)], axis=1)
    route = jnp.concatenate([meta_in[i] for i in range(PLANE)], axis=0)

    wait_bytes(dbuf.at[pl.ds(0, hsplit - 1)], one_recv.at[3])
    halves = []
    for half in range(hsplit // PLANE):
        acc = dbuf[half * PLANE].astype(F32)
        for j in range(1, PLANE):
            acc = acc + dbuf[half * PLANE + j].astype(F32)
        halves.append(acc)
    proj = jnp.concatenate(halves, axis=1).astype(BF16).astype(F32)
    resid = stream + proj
    resid_ref[...] = resid
    ssq = jnp.sum(resid * resid, axis=1, keepdims=True)
    lane8 = lax.broadcasted_iota(jnp.int32, (8, LANES), 1)
    meta_blk[...] = jnp.where(lane8 == 2 * RESIDENT, ssq, route)
    meta_all[h] = meta_blk[...]
    yblk[...] = (resid * gain_row).astype(BF16)
    xbuf[h] = yblk[...]

    def spread(i):
        target = m * hsplit + lax.rem(h + i, hsplit)
        copy_to(meta_blk, meta_all.at[h], one_send.at[4], one_recv.at[4], target).start()
        copy_to(yblk, xbuf.at[h], one_send.at[5], one_recv.at[5], target).start()

    each(hsplit, spread, 1)
    wait_bytes(meta_all.at[pl.ds(0, hsplit - 1)], one_recv.at[4])

    info = meta_all[...].reshape(batch, LANES)
    info_t = info.T
    ia = lax.broadcasted_iota(jnp.int32, (batch, batch), 0)
    ib = lax.broadcasted_iota(jnp.int32, (batch, batch), 1)
    before_t = jnp.where(ia < ib, 1.0, 0.0).astype(BF16)
    before = jnp.where(ib < ia, 1.0, 0.0).astype(BF16)
    ranks_t = nn_dot(info_t[0:8].astype(BF16), before_t)
    ranks = nn_dot(before, info.astype(BF16))

    def place_of(rank, picked):
        out = rank
        for c in range(1, quarters):
            step = float(c * pad - edges[c] - (c - 1) * pad + edges[c - 1])
            if step:
                out = out + jnp.where(rank >= float(edges[c]), step, 0.0)
        return jnp.where(picked > 0.5, out, -1.0)

    rows_i = [place_of(ranks_t[RESIDENT + e : RESIDENT + e + 1], info_t[RESIDENT + e : RESIDENT + e + 1]) for e in range(RESIDENT)]
    cols_i = [place_of(ranks[:, RESIDENT + e : RESIDENT + e + 1], info[:, RESIDENT + e : RESIDENT + e + 1]) for e in range(RESIDENT)]
    ssq_row[...] = info_t[2 * RESIDENT : 2 * RESIDENT + 1]
    ssq_all[m] = ssq_row[...]

    def ssq_send(i):
        j = lax.rem(m + i, MSPLIT)
        copy_to(ssq_row, ssq_all.at[m], one_send.at[6], one_recv.at[6], j * hsplit + low).start()

    each(MSPLIT, ssq_send, 1)

    wait_bytes(xbuf.at[pl.ds(0, hsplit - 1)], one_recv.at[5])
    x = xbuf[...].reshape(batch, bw)
    r_iota = lax.broadcasted_iota(jnp.int32, (rows, batch), 0).astype(F32)
    for e in range(RESIDENT):
        pick = jnp.where(r_iota == rows_i[e], 1.0, 0.0).astype(BF16)
        xcs[e] = nn_dot(pick, x).astype(BF16)
    loads[2].wait()
    loads[3].wait()

    fwd = MSPLIT // 2
    bwd = MSPLIT - 1 - fwd

    def ring(step):
        return lax.rem(m + sgn * step + 2 * MSPLIT, MSPLIT)

    next_dev = ring(1) * hsplit + low
    prev_dev = ring(-1) * hsplit + low

    def sized(chunk, body):
        odd = lax.rem(chunk, 2)

        @pl.when(odd == 0)
        def _():
            body(pl.ds(0, pad), 0)

        @pl.when(odd == 1)
        def _():
            body(pl.ds(0, short), 1)

    def rs_start(slot, q, chunk, target):
        def go(r, kind):
            copy_to(
                rs_send.at[slot, q, r],
                rs_recv.at[slot, q, r],
                size_send.at[kind],
                rs_sem.at[slot, q],
                target,
            ).start()

        sized(chunk, go)

    def rs_wait(slot, q, chunk):
        sized(chunk, lambda r, kind: wait_bytes(rs_recv.at[slot, q, r], rs_sem.at[slot, q]))

    def first(q):
        cols = pl.ds(pl.multiple_of(q * LANES, LANES), LANES)
        for e in range(RESIDENT):
            rhs = jnp.concatenate([gbuf[e, :, cols], ubuf[e, :, cols]], axis=1)
            r = nn_dot(xcs[e], rhs)
            own[q, e * quarters : (e + 1) * quarters] = r.reshape(quarters, pad, 2 * LANES)
        rs_send[0, q] = own[q, ring(fwd)].astype(BF16)
        rs_start(0, q, ring(fwd), next_dev)
        rs_send[fwd, q] = own[q, ring(-bwd)].astype(BF16)
        rs_start(fwd, q, ring(-bwd), prev_dev)

    each(pieces, first)

    for t in range(1, fwd):

        def onward(q, t=t):
            chunk = ring(fwd - t)
            rs_wait(t - 1, q, chunk)
            v = rs_recv[t - 1, q].astype(F32) + own[q, chunk]
            rs_send[t, q] = v.astype(BF16)
            rs_start(t, q, chunk, next_dev)
            if t < bwd:
                b = fwd + t
                chunk = ring(t - bwd)
                rs_wait(b - 1, q, chunk)
                v = rs_recv[b - 1, q].astype(F32) + own[q, chunk]
                rs_send[b, q] = v.astype(BF16)
                rs_start(b, q, chunk, prev_dev)

        each(pieces, onward)

    wait_bytes(ssq_all.at[pl.ds(0, MSPLIT - 1)], one_recv.at[6])
    power = ssq_all[0]
    for j in range(1, MSPLIT):
        power = power + ssq_all[j]
    chunk_row = jnp.where(m < quarters, rows_i[0], rows_i[1])
    c_iota = lax.broadcasted_iota(jnp.int32, (pad, batch), 0) + lax.rem(m, quarters) * pad
    hit = c_iota.astype(F32) == chunk_row
    mean = jnp.sum(jnp.where(hit, power, 0.0), axis=1, keepdims=True) / float(width)
    factor = lax.rsqrt(mean + 1e-05)

    def ag_start(slot, q, chunk, target):
        def go(r, kind):
            copy_to(
                hbuf.at[q, chunk, r],
                hbuf.at[q, chunk, r],
                size_send.at[2 + kind],
                ag_sem.at[slot, q],
                target,
            ).start()

        sized(chunk, go)

    def ag_wait(slot, q, chunk):
        sized(chunk, lambda r, kind: wait_bytes(hbuf.at[q, chunk, r], ag_sem.at[slot, q]))

    def finish(q):
        rs_wait(fwd - 1, q, m)
        rs_wait(MSPLIT - 2, q, m)
        v = own[q, m] + rs_recv[fwd - 1, q].astype(F32) + rs_recv[MSPLIT - 2, q].astype(F32)
        v = v * factor
        ga = v[:, :LANES]
        up_half = v[:, LANES:]
        hbuf[q, m] = (ga / (1.0 + jnp.exp(-ga)) * up_half).astype(BF16)
        ag_start(0, q, m, next_dev)
        ag_start(fwd, q, m, prev_dev)

    each(pieces, finish)

    for t in range(1, fwd):

        def relay(q, t=t):
            ag_wait(t - 1, q, ring(-t))
            ag_start(t, q, ring(-t), next_dev)
            if t < bwd:
                b = fwd + t
                ag_wait(b - 1, q, ring(t))
                ag_start(b, q, ring(t), prev_dev)

        each(pieces, relay)

    def arrived(q):
        ag_wait(fwd - 1, q, ring(-fwd))
        ag_wait(MSPLIT - 2, q, ring(bwd))

    each(pieces, arrived)

    loads[4].wait()
    col_iota = lax.broadcasted_iota(jnp.int32, (batch, rows), 1).astype(F32)
    row_iota = lax.broadcasted_iota(jnp.int32, (rows, LANES), 0)
    filled = lax.rem(row_iota, 2 * pad) < pad + short
    spreads = []
    for e in range(RESIDENT):
        hc = jnp.concatenate(
            [
                jnp.where(
                    filled,
                    hbuf[q, e * quarters : (e + 1) * quarters].astype(F32).reshape(rows, LANES),
                    0.0,
                ).astype(BF16)
                for q in range(pieces)
            ],
            axis=1,
        )
        pick = jnp.where(col_iota == cols_i[e], 1.0, 0.0).astype(BF16)
        spreads.append(nn_dot(pick, hc).astype(BF16))
    tile = 256
    for c in range(bw // tile):
        cols = slice(c * tile, (c + 1) * tile)
        total = jnp.zeros((batch, tile), F32)
        for e in range(RESIDENT):
            total = total + info[:, e : e + 1] * nn_dot(spreads[e], dwbuf[e, :, cols])
        kout[:, :, cols] = total.astype(BF16).reshape(hsplit, 8, tile)

    def ffn_send(i):
        j = lax.rem(h + i, hsplit)
        copy_to(kout.at[j], kin.at[h], one_send.at[9], one_recv.at[7], m * hsplit + j).start()

    each(hsplit, ffn_send, 1)
    kin[h] = kout[h]
    wait_bytes(kin.at[pl.ds(0, hsplit - 1)], one_recv.at[7])
    ffn = kin[0].astype(F32)
    for j in range(1, hsplit):
        ffn = ffn + kin[j].astype(F32)
    final = resid_ref[...] + ffn
    for c in range(8):
        lf[pl.ds(c, 8, stride=8), :] = final[:, c * LANES : (c + 1) * LANES]
    lout[...] = lf[...].reshape(PLANE, 8, LANES).astype(BF16)

    def row_send(i):
        target = h * PLANE + i

        @pl.when(target != me)
        def _():
            copy_to(lout.at[i], lbuf.at[m], l_send.at[i], l_recv.at[m], target).start()

    each(PLANE, row_send)

    @pl.when(z == h)
    def _():
        lbuf[m] = lout[k]

    wait_bytes(abuf.at[0, pl.ds(0, PLANE - 1)], one_send.at[0])
    wait_bytes(wbuf.at[pl.ds(0, PLANE - 1)], one_send.at[1])
    wait_bytes(abuf.at[pl.ds(0, planes - 1)], one_send.at[2])
    wait_bytes(dbuf.at[pl.ds(0, hsplit - 1)], one_send.at[3])
    wait_bytes(meta_all.at[pl.ds(0, hsplit - 1)], one_send.at[4])
    wait_bytes(xbuf.at[pl.ds(0, hsplit - 1)], one_send.at[5])
    wait_bytes(ssq_all.at[pl.ds(0, MSPLIT - 1)], one_send.at[6])
    for parity in range(2):

        @pl.when(lax.rem(m, 2) == parity)
        def _(parity=parity):
            rs_even = MSPLIT // 2 - (1 - parity)
            ag_steps = list(range(fwd)) + list(range(bwd))
            ag_even = sum((parity + step) % 2 == 0 for step in ag_steps)
            wait_bytes(rs_send.at[pl.ds(0, rs_even)], size_send.at[0])
            wait_bytes(rs_send.at[pl.ds(0, hops - rs_even), :, pl.ds(0, short)], size_send.at[1])
            wait_bytes(hbuf.at[:, pl.ds(0, ag_even)], size_send.at[2])
            wait_bytes(hbuf.at[:, pl.ds(0, hops - ag_even), pl.ds(0, short)], size_send.at[3])

    wait_bytes(kin.at[pl.ds(0, hsplit - 1)], one_send.at[9])

    def drain(j):
        @pl.when(j * hsplit + z != me)
        def _():
            wait_bytes(sblk.at[j], st_send.at[j])
            wait_bytes(meta_out, me_send.at[j])
            wait_bytes(lbuf.at[j], l_recv.at[j])

        @pl.when(h * PLANE + j != me)
        def _():
            wait_bytes(lout.at[j], l_send.at[j])

    each(MSPLIT, drain)

    qf[...] = lbuf[...].reshape(MSPLIT * 8, LANES).astype(F32)
    for j in range(width // LANES):
        out_ref[0:1, j * LANES : (j + 1) * LANES] = qf[j : j + 1, :]


def on_device(
    stream_in,
    query,
    key_new,
    value_new,
    key_cache,
    value_cache,
    lengths,
    route_ids,
    route_scores,
    out_weight,
    norm_gain,
    gate_weight,
    up_weight,
    down_weight,
):
    n = lax.axis_size("gx")
    width = stream_in.shape[1]
    slots = key_cache.shape[1]
    kv = key_cache.shape[2]
    hidden = gate_weight.shape[2]
    bw = width // MSPLIT
    hsplit = n // MSPLIT
    planes = n // PLANE
    cols = out_weight.shape[1]
    quarters = MSPLIT // RESIDENT
    cap = 5 * n // 8
    edges = [-(-(cap * c // quarters) // 8) * 8 for c in range(quarters + 1)]
    pad = edges[1] - edges[0]
    short = edges[2] - edges[1]
    assert [b - a for a, b in zip(edges, edges[1:])] == [pad, short] * (quarters // 2)
    pieces = hidden // LANES
    cfg = dict(n=n, width=width, hidden=hidden, edges=edges, pad=pad, short=short)
    hops = MSPLIT - 1

    def vmem(*shape, dtype=BF16):
        return pltpu.VMEM(shape, dtype)

    scratch = [
        vmem(slots, kv),
        vmem(slots, kv),
        vmem(*gate_weight.shape),
        vmem(*up_weight.shape),
        vmem(*down_weight.shape),
        vmem(PLANE, cols, bw),
        vmem(width // LANES, LANES, dtype=F32),
        vmem(width // LANES, LANES, dtype=F32),
        vmem(MSPLIT, 8, LANES),
        vmem(KVH, 8, HS),
        vmem(planes, PLANE, 8, HS),
        vmem(n * 8, LANES, dtype=F32),
        vmem(hsplit, 8, PLANE * cols),
        vmem(hsplit, 8, PLANE * cols),
        vmem(PLANE, 8, LANES),
        vmem(1, LANES, dtype=F32),
        vmem(PLANE, 1, LANES, dtype=F32),
        vmem(8, LANES, dtype=F32),
        vmem(hsplit, 8, LANES, dtype=F32),
        vmem(8, bw, dtype=F32),
        vmem(8, bw),
        vmem(hsplit, 8, bw),
        vmem(1, LANES, dtype=F32),
        vmem(MSPLIT, 1, LANES, dtype=F32),
        vmem(RESIDENT, quarters * pad, bw),
        vmem(pieces, MSPLIT, pad, 2 * LANES, dtype=F32),
        vmem(hops, pieces, pad, 2 * LANES),
        vmem(hops, pieces, pad, 2 * LANES),
        vmem(pieces, MSPLIT, pad, LANES),
        vmem(hsplit, 8, bw),
        vmem(hsplit, 8, bw),
        vmem(PLANE * 8, LANES, dtype=F32),
        vmem(PLANE, 8, LANES),
        vmem(MSPLIT, 8, LANES),
        vmem(1, width),
        vmem(1, width),
        vmem(1, kv),
        vmem(1, kv),
        vmem(width // LANES, LANES, dtype=F32),
        pltpu.SemaphoreType.DMA((11,)),
        pltpu.SemaphoreType.DMA((10,)),
        pltpu.SemaphoreType.DMA((8,)),
        pltpu.SemaphoreType.DMA((planes,)),
        pltpu.SemaphoreType.REGULAR((4,)),
        pltpu.SemaphoreType.DMA((4,)),
        pltpu.SemaphoreType.DMA((MSPLIT,)),
        pltpu.SemaphoreType.DMA((PLANE,)),
        pltpu.SemaphoreType.DMA((MSPLIT,)),
        pltpu.SemaphoreType.DMA((PLANE,)),
        pltpu.SemaphoreType.DMA((hops, pieces)),
        pltpu.SemaphoreType.DMA((hops, pieces)),
        pltpu.SemaphoreType.DMA((PLANE,)),
        pltpu.SemaphoreType.DMA((MSPLIT,)),
    ]
    smem = pl.BlockSpec(memory_space=pltpu.SMEM)
    local = pl.BlockSpec(memory_space=pltpu.VMEM)
    anywhere = pl.BlockSpec(memory_space=pl.ANY)
    return pl.pallas_call(
        functools.partial(layer_kernel, cfg),
        out_shape=jax.ShapeDtypeStruct((1, width), F32),
        in_specs=[smem] * 3 + [anywhere] * 11,
        out_specs=local,
        scratch_shapes=scratch,
        compiler_params=pltpu.CompilerParams(
            collective_id=0, has_side_effects=True, vmem_limit_bytes=60 * 1024 * 1024
        ),
        name="layer",
    )(
        lengths,
        route_ids,
        route_scores,
        stream_in,
        query,
        key_new,
        value_new,
        norm_gain.reshape(width // LANES, LANES),
        key_cache.reshape(slots, kv),
        value_cache.reshape(slots, kv),
        out_weight.T,
        gate_weight,
        up_weight,
        down_weight,
    ).astype(BF16)


def solution(mesh):
    rows = P(("groups", "gx"), None)
    in_specs = (
        rows,
        rows,
        rows,
        rows,
        P(("groups", "gx"), None, None),
        P(("groups", "gx"), None, None),
        P(("groups", "gx")),
        rows,
        rows,
        P(None, "gx"),
        P(),
        P(None, "gx", None),
        P(None, "gx", None),
        P(None, "gx", None),
    )
    return jax.shard_map(
        on_device, mesh=mesh, in_specs=in_specs, out_specs=rows, check_vma=False
    )
```

```python
import functools

import jax
import jax.numpy as jnp
from jax import lax
from jax.experimental import pallas as pl
from jax.experimental.pallas import tpu as pltpu
from jax.sharding import PartitionSpec as P

NH = 64
KVH = 8
HS = 128
RESIDENT = 2
MSPLIT = 8
PLANE = 8
LANES = 128
BF16 = jnp.bfloat16
F32 = jnp.float32
MESH = pl.DeviceIdType.MESH


def nt_dot(a, b):
    return lax.dot_general(a, b, (((1,), (1,)), ((), ())), preferred_element_type=F32)


def nn_dot(a, b):
    return lax.dot_general(a, b, (((1,), (0,)), ((), ())), preferred_element_type=F32)


def copy_to(src, dst, send, recv, target):
    return pltpu.make_async_remote_copy(
        src_ref=src,
        dst_ref=dst,
        send_sem=send,
        recv_sem=recv,
        device_id={"gx": target},
        device_id_type=MESH,
    )


def wait_bytes(ref, sem):
    pltpu.make_async_copy(ref, ref, sem).wait()


def each(count, body, start=0):
    def step(i, carry):
        body(i)
        return carry

    lax.fori_loop(start, count, step, 0)


def layer_kernel(
    cfg,
    lengths_in,
    ids_in,
    scores_in,
    stream_in,
    query,
    key_new,
    value_new,
    gain,
    key_cache,
    value_cache,
    out_weight,
    gate_weight,
    up_weight,
    down_weight,
    out_ref,
    kbuf,
    vbuf,
    gbuf,
    ubuf,
    dwbuf,
    wbuf,
    qf,
    sf,
    sblk,
    att,
    abuf,
    af,
    pbuf,
    dbuf,
    sbuf,
    meta_out,
    meta_in,
    meta_blk,
    meta_all,
    resid_ref,
    yblk,
    xbuf,
    ssq_row,
    ssq_all,
    xcs,
    own,
    rs_send,
    rs_recv,
    hbuf,
    kout,
    kin,
    lf,
    lout,
    lbuf,
    svm,
    qvm,
    knvm,
    vnvm,
    gainvm,
    lengths,
    route_ids,
    route_scores,
    pst,
    pme,
    route_blk,
    route_all,
    acc,
    picks,
    loc_sem,
    one_send,
    one_recv,
    z_recv,
    tok,
    size_send,
    st_send,
    st_recv,
    me_send,
    me_recv,
    rs_sem,
    ag_sem,
    l_send,
    l_recv,
):
    n = cfg["n"]
    hsplit = n // MSPLIT
    planes = n // PLANE
    batch = n
    width = cfg["width"]
    bw = width // MSPLIT
    pieces = cfg["hidden"] // LANES
    edges = cfg["edges"]
    pad = cfg["pad"]
    short = cfg["short"]
    quarters = MSPLIT // RESIDENT
    rows = quarters * pad
    hops = MSPLIT - 1

    me = lax.axis_index("gx")
    z = me // PLANE
    k = lax.rem(me, PLANE)
    m = me // hsplit
    h = lax.rem(me, hsplit)
    low = me - m * hsplit
    sgn = 1 - 2 * lax.rem(me, 2)

    def up(step):
        return lax.rem(z + sgn * step + 2 * planes, planes)

    def signal(sem, target):
        pl.semaphore_signal(sem, inc=1, device_id={"gx": target}, device_id_type=MESH)

    small = [
        pltpu.make_async_copy(src, dst, loc_sem.at[6 + i])
        for i, (src, dst) in enumerate(
            [
                (query, qvm),
                (key_new, knvm),
                (value_new, vnvm),
                (lengths_in, lengths),
                (stream_in, svm),
                (gain, gainvm),
                (ids_in, route_ids),
                (scores_in, route_scores),
            ]
        )
    ]
    for load in small:
        load.start()
    loads = [
        pltpu.make_async_copy(key_cache, kbuf, loc_sem.at[0]),
        pltpu.make_async_copy(value_cache, vbuf, loc_sem.at[1]),
        pltpu.make_async_copy(gate_weight, gbuf, loc_sem.at[2]),
        pltpu.make_async_copy(up_weight, ubuf, loc_sem.at[3]),
        pltpu.make_async_copy(down_weight, dwbuf, loc_sem.at[4]),
        pltpu.make_async_copy(
            out_weight.at[:, pl.ds(pl.multiple_of(k * bw, bw), bw)], wbuf.at[k], loc_sem.at[5]
        ),
    ]
    for load in loads[:2]:
        load.start()

    xs = k // 2
    core = lax.rem(k, 2)

    def peer(dx, dc):
        return 2 * lax.rem(xs + dx, PLANE // 2) + lax.rem(core + dc, 2)

    plane_steps = [(dx, dc) for dx in (2, 3, 1) for dc in (0, 1)] + [(0, 1)]
    patch_steps = [(dz, dx, dc) for dx in (2, 3, 1) for dz in (1, 0) for dc in (0, 1)]
    patch_steps += [(1, 0, 0), (1, 0, 1), (0, 0, 1)]

    def patch_peer(step):
        dz, dx, dc = step
        return lax.rem(h // PLANE + dz, 2) * PLANE + peer(dx, dc)

    barrier = pltpu.get_barrier_semaphore()

    for step in (1, -1):
        signal(barrier, up(step) * PLANE + k)

    def greet(i):
        signal(barrier, z * PLANE + lax.rem(k + i, PLANE))

    each(PLANE, greet, 1)

    for load in loads[2:]:
        load.start()

    for load in small[:4]:
        load.wait()
    for j in range(width // LANES):
        qf[j : j + 1, :] = qvm[0:1, j * LANES : (j + 1) * LANES].astype(F32)

    def per_group(row_ref):
        return jnp.concatenate(
            [
                jnp.broadcast_to(row_ref[0:1, g * HS : (g + 1) * HS].astype(F32), (NH // KVH, HS))
                for g in range(KVH)
            ],
            axis=0,
        )

    q_all = qf[...]
    scale = HS ** (-0.5)
    o = jnp.sum(q_all * per_group(knvm), axis=1, keepdims=True) * scale
    v_own = per_group(vnvm)
    loads[0].wait()
    slots = kbuf.shape[0]
    s = jnp.concatenate(
        [
            nt_dot(q_all[g * 8 : (g + 1) * 8].astype(BF16), kbuf[:, g * HS : (g + 1) * HS])
            for g in range(KVH)
        ],
        axis=0,
    )
    live = lax.broadcasted_iota(jnp.int32, (NH, slots), 1) < lengths[0]
    s = jnp.where(live, s * scale, -1e30)
    t = jnp.maximum(jnp.max(s, axis=1, keepdims=True), o)
    es = jnp.exp(s - t)
    eo = jnp.exp(o - t)
    total = jnp.sum(es, axis=1, keepdims=True) + eo
    p = es / total
    own_term = (eo / total).astype(BF16).astype(F32) * v_own
    loads[1].wait()
    for g in range(KVH):
        r = slice(g * 8, (g + 1) * 8)
        mixed = nn_dot(p[r].astype(BF16), vbuf[:, g * HS : (g + 1) * HS])
        att[g] = (mixed + own_term[r]).astype(BF16)

    pl.semaphore_wait(barrier, PLANE + 1)
    for step in (1, -1):
        signal(tok.at[0], up(step) * PLANE + k)

    for step in plane_steps:
        j = peer(*step)
        copy_to(
            att.at[j], abuf.at[z, k], one_send.at[0], one_recv.at[0], z * PLANE + j
        ).start()

    abuf[z, k] = att[k]
    for step in plane_steps:
        signal(tok.at[3], z * PLANE + peer(*step))

    pl.semaphore_wait(tok.at[0], 2)
    for step in (2, -2):
        signal(tok.at[1], up(step) * PLANE + k)

    for load in small[4:]:
        load.wait()
    for j in range(width // LANES):
        sf[j : j + 1, :] = svm[0:1, j * LANES : (j + 1) * LANES].astype(F32)
    sblk[...] = sf[...].reshape(MSPLIT, 8, LANES).astype(BF16)
    lane = lax.broadcasted_iota(jnp.int32, (1, LANES), 1)
    s0 = jnp.full((1, LANES), route_scores[0, 0], F32)
    s1 = jnp.full((1, LANES), route_scores[0, 1], F32)
    top = jnp.maximum(s0, s1)
    e0 = jnp.exp(s0 - top)
    e1 = jnp.exp(s1 - top)
    q0 = e0 / (e0 + e1)
    q1 = e1 / (e0 + e1)
    id0 = jnp.full((1, LANES), route_ids[0, 0], jnp.int32)
    id1 = jnp.full((1, LANES), route_ids[0, 1], jnp.int32)
    meta = jnp.zeros((1, LANES), F32)
    for e in range(RESIDENT):
        w = jnp.where(id0 == e, q0, 0.0) + jnp.where(id1 == e, q1, 0.0)
        w = w.astype(BF16).astype(F32)
        picked = jnp.where((id0 == e) | (id1 == e), 1.0, 0.0)
        meta = jnp.where(lane == e, w, meta)
        meta = jnp.where(lane == RESIDENT + e, picked, meta)
    meta_out[...] = meta

    gatherer = lax.rem(z, PLANE)

    @pl.when(k != gatherer)
    def _():
        target = z * PLANE + gatherer
        copy_to(sblk, pst.at[:, k], st_send.at[0], st_recv.at[0], target).start()
        copy_to(meta_out, pme.at[k], me_send.at[0], me_recv.at[0], target).start()

    @pl.when(k == gatherer)
    def _():
        for j in range(MSPLIT):
            pst[j, k] = sblk[j]
        pme[k] = meta_out[...]

    pl.semaphore_wait(tok.at[3], PLANE - 1)
    for step in plane_steps:
        j = peer(*step)
        copy_to(
            out_weight.at[:, pl.ds(pl.multiple_of(j * bw, bw), bw)],
            wbuf.at[k],
            one_send.at[1],
            one_recv.at[1],
            z * PLANE + j,
        ).start()

    wait_bytes(abuf.at[0, pl.ds(0, PLANE - 1)], one_recv.at[0])
    pl.semaphore_wait(tok.at[1], 2)

    def z_copy(origin, step):
        return copy_to(
            abuf.at[origin],
            abuf.at[origin],
            one_send.at[2],
            z_recv.at[origin],
            up(step) * PLANE + k,
        )

    reach = planes // 4
    for step in range(reach, 0, -1):
        z_copy(z, step).start()
        z_copy(z, -step).start()
    for step in (reach, -reach):
        signal(tok.at[2], up(step) * PLANE + k)
    @pl.when(k == gatherer)
    def _():
        pl.semaphore_wait(tok.at[2], 2)
        wait_bytes(pst.at[pl.ds(0, PLANE - 1)], st_recv.at[0])
        wait_bytes(pme.at[pl.ds(0, PLANE - 1)], me_recv.at[0])

        def hand_on(j):
            target = j * hsplit + z

            @pl.when(target != me)
            def _():
                copy_to(pst.at[j], sbuf, st_send.at[1], st_recv.at[1], target).start()
                copy_to(pme, meta_in, me_send.at[1], me_recv.at[1], target).start()

            @pl.when(target == me)
            def _():
                sbuf[...] = pst[j]
                meta_in[...] = pme[...]

        each(MSPLIT, hand_on)

    far = up(-reach)
    wait_bytes(abuf.at[far], z_recv.at[far])
    for step in range(reach, 0, -1):
        z_copy(far, step).start()
    near = up(reach)
    wait_bytes(abuf.at[near], z_recv.at[near])
    for step in range(reach - 1, 0, -1):
        z_copy(near, -step).start()
    @pl.when(k != gatherer)
    def _():
        pl.semaphore_wait(tok.at[2], 2)

    def z_wait(i):
        origin = lax.rem(z + i, planes)

        @pl.when((origin != far) & (origin != near))
        def _():
            wait_bytes(abuf.at[origin], z_recv.at[origin])

    each(planes, z_wait, 1)

    loads[5].wait()
    wait_bytes(wbuf.at[pl.ds(0, PLANE - 1)], one_recv.at[1])

    af[...] = abuf[...].reshape(batch * 8, LANES).astype(F32)
    a = jnp.concatenate(
        [af[pl.ds(j, batch, stride=8), :] for j in range(8)], axis=1
    ).astype(BF16)
    part = nt_dot(a, wbuf[...].reshape(PLANE * wbuf.shape[1], bw))
    pbuf[...] = part.astype(BF16).reshape(hsplit, 8, part.shape[1])

    for step in patch_steps:
        j = patch_peer(step)
        copy_to(pbuf.at[j], dbuf.at[h], one_send.at[3], one_recv.at[3], m * hsplit + j).start()
    dbuf[h] = pbuf[h]

    @pl.when(z != h)
    def _():
        wait_bytes(sbuf, st_recv.at[1])
        wait_bytes(meta_in, me_recv.at[1])

    route_blk[...] = jnp.concatenate([meta_in[i] for i in range(PLANE)], axis=0)
    route_all[h] = route_blk[...]
    for step in patch_steps:
        target = m * hsplit + patch_peer(step)
        copy_to(route_blk, route_all.at[h], one_send.at[10], one_recv.at[8], target).start()
    lf[...] = sbuf[...].reshape(PLANE * 8, LANES).astype(F32)
    stream = jnp.concatenate([lf[pl.ds(c, 8, stride=8), :] for c in range(8)], axis=1)
    g8 = gainvm[pl.ds(pl.multiple_of(m * 8, 8), 8), :]
    gain_row = jnp.concatenate([g8[c : c + 1, :] for c in range(8)], axis=1)

    wait_bytes(dbuf.at[pl.ds(0, hsplit - 1)], one_recv.at[3])
    halves = []
    for half in range(hsplit // PLANE):
        part_sum = dbuf[half * PLANE].astype(F32)
        for j in range(1, PLANE):
            part_sum = part_sum + dbuf[half * PLANE + j].astype(F32)
        halves.append(part_sum)
    proj = jnp.concatenate(halves, axis=1).astype(BF16).astype(F32)
    resid = stream + proj
    resid_ref[...] = resid
    yblk[...] = (resid * gain_row).astype(BF16)
    xbuf[h] = yblk[...]
    for step in patch_steps:
        target = m * hsplit + patch_peer(step)
        copy_to(yblk, xbuf.at[h], one_send.at[5], one_recv.at[5], target).start()
    ssq = jnp.sum(resid * resid, axis=1, keepdims=True)
    meta_blk[...] = jnp.broadcast_to(ssq, (8, LANES))
    meta_all[h] = meta_blk[...]
    for step in patch_steps:
        target = m * hsplit + patch_peer(step)
        copy_to(meta_blk, meta_all.at[h], one_send.at[4], one_recv.at[4], target).start()

    wait_bytes(route_all.at[pl.ds(0, hsplit - 1)], one_recv.at[8])
    info = route_all[...].reshape(batch, LANES)
    info_t = info.T
    ia = lax.broadcasted_iota(jnp.int32, (batch, batch), 0)
    ib = lax.broadcasted_iota(jnp.int32, (batch, batch), 1)
    before_t = jnp.where(ia < ib, 1.0, 0.0).astype(BF16)
    before = jnp.where(ib < ia, 1.0, 0.0).astype(BF16)
    ranks_t = nn_dot(info_t[0:8].astype(BF16), before_t)
    ranks = nn_dot(before, info.astype(BF16))

    def place_of(rank, picked):
        out = rank
        for c in range(1, quarters):
            step = float(c * pad - edges[c] - (c - 1) * pad + edges[c - 1])
            if step:
                out = out + jnp.where(rank >= float(edges[c]), step, 0.0)
        return jnp.where(picked > 0.5, out, -1.0)

    rows_i = [place_of(ranks_t[RESIDENT + e : RESIDENT + e + 1], info_t[RESIDENT + e : RESIDENT + e + 1]) for e in range(RESIDENT)]
    cols_i = [place_of(ranks[:, RESIDENT + e : RESIDENT + e + 1], info[:, RESIDENT + e : RESIDENT + e + 1]) for e in range(RESIDENT)]
    wait_bytes(xbuf.at[pl.ds(0, hsplit - 1)], one_recv.at[5])
    x = xbuf[...].reshape(batch, bw)
    r_iota = lax.broadcasted_iota(jnp.int32, (rows, batch), 0).astype(F32)
    for e in range(RESIDENT):
        pick = jnp.where(r_iota == rows_i[e], 1.0, 0.0).astype(BF16)
        xcs[e] = nn_dot(pick, x).astype(BF16)
    loads[2].wait()
    loads[3].wait()

    fwd = MSPLIT // 2
    bwd = MSPLIT - 1 - fwd

    def ring(q, step):
        turn = sgn * (1 - 2 * (q // fwd))
        return lax.rem(m + turn * step + 2 * MSPLIT, MSPLIT)

    def ring_dev(q, step):
        return ring(q, step) * hsplit + low

    def sized(chunk, body):
        odd = lax.rem(chunk, 2)

        @pl.when(odd == 0)
        def _():
            body(pl.ds(0, pad), 0)

        @pl.when(odd == 1)
        def _():
            body(pl.ds(0, short), 1)

    def rs_start(slot, q, chunk, target):
        def go(r, kind):
            copy_to(
                rs_send.at[slot, q, r],
                rs_recv.at[slot, q, r],
                size_send.at[kind],
                rs_sem.at[slot, q],
                target,
            ).start()

        sized(chunk, go)

    def rs_wait(slot, q, chunk):
        sized(chunk, lambda r, kind: wait_bytes(rs_recv.at[slot, q, r], rs_sem.at[slot, q]))

    def first(q):
        cols = pl.ds(pl.multiple_of(q * LANES, LANES), LANES)
        for e in range(RESIDENT):
            rhs = jnp.concatenate([gbuf[e, :, cols], ubuf[e, :, cols]], axis=1)
            r = nn_dot(xcs[e], rhs)
            own[q, e * quarters : (e + 1) * quarters] = r.reshape(quarters, pad, 2 * LANES)
        rs_send[0, q] = own[q, ring(q, fwd)].astype(BF16)
        rs_start(0, q, ring(q, fwd), ring_dev(q, 1))
        rs_send[fwd, q] = own[q, ring(q, -bwd)].astype(BF16)
        rs_start(fwd, q, ring(q, -bwd), ring_dev(q, -1))

    each(pieces, first)

    wait_bytes(meta_all.at[pl.ds(0, hsplit - 1)], one_recv.at[4])
    ssq_row[...] = meta_all[...].reshape(batch, LANES).T[0:1]
    ssq_all[m] = ssq_row[...]

    def ssq_send(i):
        j = lax.rem(m + i, MSPLIT)
        copy_to(ssq_row, ssq_all.at[m], one_send.at[6], one_recv.at[6], j * hsplit + low).start()

    each(MSPLIT, ssq_send, 1)

    for t in range(1, fwd):

        def onward(q, t=t):
            chunk = ring(q, fwd - t)
            rs_wait(t - 1, q, chunk)
            v = rs_recv[t - 1, q].astype(F32) + own[q, chunk]
            rs_send[t, q] = v.astype(BF16)
            rs_start(t, q, chunk, ring_dev(q, 1))
            if t < bwd:
                b = fwd + t
                chunk = ring(q, t - bwd)
                rs_wait(b - 1, q, chunk)
                v = rs_recv[b - 1, q].astype(F32) + own[q, chunk]
                rs_send[b, q] = v.astype(BF16)
                rs_start(b, q, chunk, ring_dev(q, -1))

        each(pieces, onward)

    wait_bytes(ssq_all.at[pl.ds(0, MSPLIT - 1)], one_recv.at[6])
    power = ssq_all[0]
    for j in range(1, MSPLIT):
        power = power + ssq_all[j]
    chunk_row = jnp.where(m < quarters, rows_i[0], rows_i[1])
    c_iota = lax.broadcasted_iota(jnp.int32, (pad, batch), 0) + lax.rem(m, quarters) * pad
    hit = c_iota.astype(F32) == chunk_row
    mean = jnp.sum(jnp.where(hit, power, 0.0), axis=1, keepdims=True) / float(width)
    factor = lax.rsqrt(mean + 1e-05)

    legs = (1, 2, 3, 4, -1, -2, -3)

    def ag_start(leg, q, chunk, step):
        def go(r, kind):
            copy_to(
                hbuf.at[q, chunk, r],
                hbuf.at[q, chunk, r],
                size_send.at[2 + kind],
                ag_sem.at[legs.index(leg), q],
                ring_dev(q, step),
            ).start()

        sized(chunk, go)

    def ag_wait(leg, q):
        chunk = ring(q, -leg)
        sized(chunk, lambda r, kind: wait_bytes(hbuf.at[q, chunk, r], ag_sem.at[legs.index(leg), q]))

    def finish(q):
        rs_wait(fwd - 1, q, m)
        rs_wait(MSPLIT - 2, q, m)
        v = own[q, m] + rs_recv[fwd - 1, q].astype(F32) + rs_recv[MSPLIT - 2, q].astype(F32)
        v = v * factor
        ga = v[:, :LANES]
        up_half = v[:, LANES:]
        hbuf[q, m] = (ga / (1.0 + jnp.exp(-ga)) * up_half).astype(BF16)
        for leg in (2, -2, 1, -1):
            ag_start(leg, q, m, leg)

    each(pieces, finish)

    def relay(q):
        ag_wait(2, q)
        ag_start(4, q, ring(q, -2), 2)
        ag_start(3, q, ring(q, -2), 1)
        ag_wait(-2, q)
        ag_start(-3, q, ring(q, 2), -1)

    each(pieces, relay)

    loads[4].wait()
    col_iota = lax.broadcasted_iota(jnp.int32, (batch, rows), 1).astype(F32)
    row_iota = lax.broadcasted_iota(jnp.int32, (rows, LANES), 0)
    filled = lax.rem(row_iota, 2 * pad) < pad + short
    for e in range(RESIDENT):
        picks[e] = jnp.where(col_iota == cols_i[e], 1.0, 0.0).astype(BF16)
    acc[...] = jnp.zeros_like(acc)

    def down(q):
        for leg in (1, -1, 3, -3, 4):
            ag_wait(leg, q)
        units = pl.ds(pl.multiple_of(q * LANES, LANES), LANES)
        for e in range(RESIDENT):
            hc = hbuf[q, e * quarters : (e + 1) * quarters].astype(F32).reshape(rows, LANES)
            hc = jnp.where(filled, hc, 0.0).astype(BF16)
            spread = nn_dot(picks[e], hc).astype(BF16)
            acc[e] += nn_dot(spread, dwbuf[e, units, :])

    each(pieces, down)
    total = info[:, 0:1] * acc[0]
    for e in range(1, RESIDENT):
        total = total + info[:, e : e + 1] * acc[e]
    kout[...] = total.astype(BF16).reshape(hsplit, 8, bw)

    for step in patch_steps:
        j = patch_peer(step)
        copy_to(kout.at[j], kin.at[h], one_send.at[9], one_recv.at[7], m * hsplit + j).start()
    kin[h] = kout[h]
    wait_bytes(kin.at[pl.ds(0, hsplit - 1)], one_recv.at[7])
    ffn = kin[0].astype(F32)
    for j in range(1, hsplit):
        ffn = ffn + kin[j].astype(F32)
    final = resid_ref[...] + ffn
    for c in range(8):
        lf[pl.ds(c, 8, stride=8), :] = final[:, c * LANES : (c + 1) * LANES]
    lout[...] = lf[...].reshape(PLANE, 8, LANES).astype(BF16)

    def row_send(i):
        target = h * PLANE + i

        @pl.when(target != me)
        def _():
            copy_to(lout.at[i], lbuf.at[m], l_send.at[i], l_recv.at[m], target).start()

    each(PLANE, row_send)

    @pl.when(z == h)
    def _():
        lbuf[m] = lout[k]

    wait_bytes(abuf.at[0, pl.ds(0, PLANE - 1)], one_send.at[0])
    wait_bytes(wbuf.at[pl.ds(0, PLANE - 1)], one_send.at[1])
    wait_bytes(abuf.at[pl.ds(0, planes - 1)], one_send.at[2])
    wait_bytes(dbuf.at[pl.ds(0, hsplit - 1)], one_send.at[3])
    wait_bytes(meta_all.at[pl.ds(0, hsplit - 1)], one_send.at[4])
    wait_bytes(xbuf.at[pl.ds(0, hsplit - 1)], one_send.at[5])
    wait_bytes(ssq_all.at[pl.ds(0, MSPLIT - 1)], one_send.at[6])
    for parity in range(2):

        @pl.when(lax.rem(m, 2) == parity)
        def _(parity=parity):
            rs_even = MSPLIT // 2 - (1 - parity)
            ag_steps = (0, 0, 0, 0, -2, -2, 2)
            ag_even = sum((parity + step) % 2 == 0 for step in ag_steps)
            wait_bytes(rs_send.at[pl.ds(0, rs_even)], size_send.at[0])
            wait_bytes(rs_send.at[pl.ds(0, hops - rs_even), :, pl.ds(0, short)], size_send.at[1])
            wait_bytes(hbuf.at[:, pl.ds(0, ag_even)], size_send.at[2])
            wait_bytes(hbuf.at[:, pl.ds(0, hops - ag_even), pl.ds(0, short)], size_send.at[3])

    wait_bytes(kin.at[pl.ds(0, hsplit - 1)], one_send.at[9])
    wait_bytes(route_all.at[pl.ds(0, hsplit - 1)], one_send.at[10])

    @pl.when(k != gatherer)
    def _():
        wait_bytes(sblk, st_send.at[0])
        wait_bytes(meta_out, me_send.at[0])

    @pl.when((k == gatherer) & (z == h))
    def _():
        wait_bytes(pst.at[pl.ds(0, MSPLIT - 1)], st_send.at[1])
        wait_bytes(route_all.at[pl.ds(0, MSPLIT - 1)], me_send.at[1])

    @pl.when((k == gatherer) & (z != h))
    def _():
        wait_bytes(pst, st_send.at[1])
        wait_bytes(route_all.at[pl.ds(0, MSPLIT)], me_send.at[1])

    def drain(j):
        @pl.when(j * hsplit + z != me)
        def _():
            wait_bytes(lbuf.at[j], l_recv.at[j])

        @pl.when(h * PLANE + j != me)
        def _():
            wait_bytes(lout.at[j], l_send.at[j])

    each(MSPLIT, drain)

    qf[...] = lbuf[...].reshape(MSPLIT * 8, LANES).astype(F32)
    for j in range(width // LANES):
        out_ref[0:1, j * LANES : (j + 1) * LANES] = qf[j : j + 1, :]


def on_device(
    stream_in,
    query,
    key_new,
    value_new,
    key_cache,
    value_cache,
    lengths,
    route_ids,
    route_scores,
    out_weight,
    norm_gain,
    gate_weight,
    up_weight,
    down_weight,
):
    n = lax.axis_size("gx")
    width = stream_in.shape[1]
    slots = key_cache.shape[1]
    kv = key_cache.shape[2]
    hidden = gate_weight.shape[2]
    bw = width // MSPLIT
    hsplit = n // MSPLIT
    planes = n // PLANE
    cols = out_weight.shape[1]
    quarters = MSPLIT // RESIDENT
    cap = 5 * n // 8
    edges = [-(-(cap * c // quarters) // 8) * 8 for c in range(quarters + 1)]
    pad = edges[1] - edges[0]
    short = edges[2] - edges[1]
    assert [b - a for a, b in zip(edges, edges[1:])] == [pad, short] * (quarters // 2)
    pieces = hidden // LANES
    cfg = dict(n=n, width=width, hidden=hidden, edges=edges, pad=pad, short=short)
    hops = MSPLIT - 1

    def vmem(*shape, dtype=BF16):
        return pltpu.VMEM(shape, dtype)

    scratch = [
        vmem(slots, kv),
        vmem(slots, kv),
        vmem(*gate_weight.shape),
        vmem(*up_weight.shape),
        vmem(*down_weight.shape),
        vmem(PLANE, cols, bw),
        vmem(width // LANES, LANES, dtype=F32),
        vmem(width // LANES, LANES, dtype=F32),
        vmem(MSPLIT, 8, LANES),
        vmem(KVH, 8, HS),
        vmem(planes, PLANE, 8, HS),
        vmem(n * 8, LANES, dtype=F32),
        vmem(hsplit, 8, PLANE * cols),
        vmem(hsplit, 8, PLANE * cols),
        vmem(PLANE, 8, LANES),
        vmem(1, LANES, dtype=F32),
        vmem(PLANE, 1, LANES, dtype=F32),
        vmem(8, LANES, dtype=F32),
        vmem(hsplit, 8, LANES, dtype=F32),
        vmem(8, bw, dtype=F32),
        vmem(8, bw),
        vmem(hsplit, 8, bw),
        vmem(1, LANES, dtype=F32),
        vmem(MSPLIT, 1, LANES, dtype=F32),
        vmem(RESIDENT, quarters * pad, bw),
        vmem(pieces, MSPLIT, pad, 2 * LANES, dtype=F32),
        vmem(hops, pieces, pad, 2 * LANES),
        vmem(hops, pieces, pad, 2 * LANES),
        vmem(pieces, MSPLIT, pad, LANES),
        vmem(hsplit, 8, bw),
        vmem(hsplit, 8, bw),
        vmem(PLANE * 8, LANES, dtype=F32),
        vmem(PLANE, 8, LANES),
        vmem(MSPLIT, 8, LANES),
        vmem(1, width),
        vmem(1, width),
        vmem(1, kv),
        vmem(1, kv),
        vmem(width // LANES, LANES, dtype=F32),
        pltpu.SMEM((1,), jnp.int32),
        pltpu.SMEM((1, 2), jnp.int32),
        pltpu.SMEM((1, 2), F32),
        vmem(MSPLIT, PLANE, 8, LANES),
        vmem(PLANE, 1, LANES, dtype=F32),
        vmem(8, LANES, dtype=F32),
        vmem(hsplit, 8, LANES, dtype=F32),
        vmem(RESIDENT, n, bw, dtype=F32),
        vmem(RESIDENT, n, quarters * pad),
        pltpu.SemaphoreType.DMA((14,)),
        pltpu.SemaphoreType.DMA((11,)),
        pltpu.SemaphoreType.DMA((9,)),
        pltpu.SemaphoreType.DMA((planes,)),
        pltpu.SemaphoreType.REGULAR((4,)),
        pltpu.SemaphoreType.DMA((4,)),
        pltpu.SemaphoreType.DMA((2,)),
        pltpu.SemaphoreType.DMA((2,)),
        pltpu.SemaphoreType.DMA((2,)),
        pltpu.SemaphoreType.DMA((2,)),
        pltpu.SemaphoreType.DMA((hops, pieces)),
        pltpu.SemaphoreType.DMA((hops, pieces)),
        pltpu.SemaphoreType.DMA((PLANE,)),
        pltpu.SemaphoreType.DMA((MSPLIT,)),
    ]
    local = pl.BlockSpec(memory_space=pltpu.VMEM)
    anywhere = pl.BlockSpec(memory_space=pl.ANY)
    return pl.pallas_call(
        functools.partial(layer_kernel, cfg),
        out_shape=jax.ShapeDtypeStruct((1, width), F32),
        in_specs=[anywhere] * 14,
        out_specs=local,
        scratch_shapes=scratch,
        compiler_params=pltpu.CompilerParams(
            collective_id=0, has_side_effects=True, vmem_limit_bytes=60 * 1024 * 1024
        ),
        name="layer",
    )(
        lengths,
        route_ids,
        route_scores,
        stream_in,
        query,
        key_new,
        value_new,
        norm_gain.reshape(width // LANES, LANES),
        key_cache.reshape(slots, kv),
        value_cache.reshape(slots, kv),
        out_weight.T,
        gate_weight,
        up_weight,
        down_weight,
    ).astype(BF16)


def solution(mesh):
    rows = P(("groups", "gx"), None)
    in_specs = (
        rows,
        rows,
        rows,
        rows,
        P(("groups", "gx"), None, None),
        P(("groups", "gx"), None, None),
        P(("groups", "gx")),
        rows,
        rows,
        P(None, "gx"),
        P(),
        P(None, "gx", None),
        P(None, "gx", None),
        P(None, "gx", None),
    )
    return jax.shard_map(
        on_device, mesh=mesh, in_specs=in_specs, out_specs=rows, check_vma=False
    )
```

```python
import functools

import jax
import jax.numpy as jnp
from jax import lax
from jax.experimental import pallas as pl
from jax.experimental.pallas import tpu as pltpu
from jax.sharding import PartitionSpec as P

NH = 64
KVH = 8
HS = 128
RESIDENT = 2
MSPLIT = 8
PLANE = 8
LANES = 128
BF16 = jnp.bfloat16
F32 = jnp.float32
MESH = pl.DeviceIdType.MESH


def nt_dot(a, b):
    return lax.dot_general(a, b, (((1,), (1,)), ((), ())), preferred_element_type=F32)


def nn_dot(a, b):
    return lax.dot_general(a, b, (((1,), (0,)), ((), ())), preferred_element_type=F32)


def copy_to(src, dst, send, recv, target):
    return pltpu.make_async_remote_copy(
        src_ref=src,
        dst_ref=dst,
        send_sem=send,
        recv_sem=recv,
        device_id={"gx": target},
        device_id_type=MESH,
    )


def wait_bytes(ref, sem):
    pltpu.make_async_copy(ref, ref, sem).wait()


def each(count, body, start=0):
    def step(i, carry):
        body(i)
        return carry

    lax.fori_loop(start, count, step, 0)


def layer_kernel(
    cfg,
    lengths_in,
    ids_in,
    scores_in,
    stream_in,
    query,
    key_new,
    value_new,
    gain,
    key_cache,
    value_cache,
    out_weight,
    gate_weight,
    up_weight,
    down_weight,
    out_ref,
    kbuf,
    vbuf,
    gbuf,
    ubuf,
    dwbuf,
    wbuf,
    qf,
    sf,
    sblk,
    att,
    abuf,
    af,
    pbuf,
    dbuf,
    sbuf,
    meta_out,
    meta_in,
    meta_blk,
    meta_all,
    resid_ref,
    yblk,
    xbuf,
    ssq_row,
    ssq_all,
    xcs,
    own,
    rs_send,
    rs_recv,
    hbuf,
    kout,
    kin,
    lf,
    lout,
    lbuf,
    svm,
    qvm,
    knvm,
    vnvm,
    gainvm,
    lengths,
    route_ids,
    route_scores,
    pst,
    pme,
    route_blk,
    route_all,
    acc,
    picks,
    loc_sem,
    one_send,
    one_recv,
    z_recv,
    tok,
    size_send,
    st_send,
    st_recv,
    me_send,
    me_recv,
    rs_sem,
    ag_sem,
    l_send,
    l_recv,
):
    n = cfg["n"]
    hsplit = n // MSPLIT
    planes = n // PLANE
    batch = n
    width = cfg["width"]
    bw = width // MSPLIT
    pieces = cfg["hidden"] // LANES
    edges = cfg["edges"]
    pad = cfg["pad"]
    short = cfg["short"]
    quarters = MSPLIT // RESIDENT
    rows = quarters * pad
    hops = MSPLIT - 1

    me = lax.axis_index("gx")
    z = me // PLANE
    k = lax.rem(me, PLANE)
    m = me // hsplit
    h = lax.rem(me, hsplit)
    low = me - m * hsplit
    sgn = 1 - 2 * lax.rem(me, 2)

    def up(step):
        return lax.rem(z + sgn * step + 2 * planes, planes)

    def signal(sem, target):
        pl.semaphore_signal(sem, inc=1, device_id={"gx": target}, device_id_type=MESH)

    small = [
        pltpu.make_async_copy(src, dst, loc_sem.at[6 + i])
        for i, (src, dst) in enumerate(
            [
                (query, qvm),
                (key_new, knvm),
                (value_new, vnvm),
                (lengths_in, lengths),
                (stream_in, svm),
                (gain, gainvm),
                (ids_in, route_ids),
                (scores_in, route_scores),
            ]
        )
    ]
    for load in small:
        load.start()
    loads = [
        pltpu.make_async_copy(key_cache, kbuf, loc_sem.at[0]),
        pltpu.make_async_copy(value_cache, vbuf, loc_sem.at[1]),
        pltpu.make_async_copy(gate_weight, gbuf, loc_sem.at[2]),
        pltpu.make_async_copy(up_weight, ubuf, loc_sem.at[3]),
        pltpu.make_async_copy(down_weight, dwbuf, loc_sem.at[4]),
        pltpu.make_async_copy(
            out_weight.at[:, pl.ds(pl.multiple_of(k * bw, bw), bw)], wbuf.at[k], loc_sem.at[5]
        ),
    ]
    for load in loads[:2]:
        load.start()

    xs = k // 2
    core = lax.rem(k, 2)

    def peer(dx, dc):
        return 2 * lax.rem(xs + dx, PLANE // 2) + lax.rem(core + dc, 2)

    plane_steps = [(dx, dc) for dx in (2, 3, 1) for dc in (0, 1)] + [(0, 1)]
    patch_steps = [(dz, dx, dc) for dx in (2, 3, 1) for dz in (1, 0) for dc in (0, 1)]
    patch_steps += [(1, 0, 0), (1, 0, 1), (0, 0, 1)]

    def patch_peer(step):
        dz, dx, dc = step
        return lax.rem(h // PLANE + dz, 2) * PLANE + peer(dx, dc)

    barrier = pltpu.get_barrier_semaphore()

    for step in (1, -1):
        signal(barrier, up(step) * PLANE + k)

    def greet(i):
        signal(barrier, z * PLANE + lax.rem(k + i, PLANE))

    each(PLANE, greet, 1)

    for load in loads[2:]:
        load.start()

    for load in small[:4]:
        load.wait()
    for j in range(width // LANES):
        qf[j : j + 1, :] = qvm[0:1, j * LANES : (j + 1) * LANES].astype(F32)

    def per_group(row_ref):
        return jnp.concatenate(
            [
                jnp.broadcast_to(row_ref[0:1, g * HS : (g + 1) * HS].astype(F32), (NH // KVH, HS))
                for g in range(KVH)
            ],
            axis=0,
        )

    q_all = qf[...]
    scale = HS ** (-0.5)
    o = jnp.sum(q_all * per_group(knvm), axis=1, keepdims=True) * scale
    v_own = per_group(vnvm)
    loads[0].wait()
    slots = kbuf.shape[0]
    s = jnp.concatenate(
        [
            nt_dot(q_all[g * 8 : (g + 1) * 8].astype(BF16), kbuf[:, g * HS : (g + 1) * HS])
            for g in range(KVH)
        ],
        axis=0,
    )
    live = lax.broadcasted_iota(jnp.int32, (NH, slots), 1) < lengths[0]
    s = jnp.where(live, s * scale, -1e30)
    t = jnp.maximum(jnp.max(s, axis=1, keepdims=True), o)
    es = jnp.exp(s - t)
    eo = jnp.exp(o - t)
    total = jnp.sum(es, axis=1, keepdims=True) + eo
    p = es / total
    own_term = (eo / total).astype(BF16).astype(F32) * v_own
    loads[1].wait()
    for g in range(KVH):
        r = slice(g * 8, (g + 1) * 8)
        mixed = nn_dot(p[r].astype(BF16), vbuf[:, g * HS : (g + 1) * HS])
        att[g] = (mixed + own_term[r]).astype(BF16)

    pl.semaphore_wait(barrier, PLANE + 1)
    for step in (1, -1):
        signal(tok.at[0], up(step) * PLANE + k)

    for step in plane_steps:
        j = peer(*step)
        copy_to(
            att.at[j], abuf.at[z, k], one_send.at[0], one_recv.at[0], z * PLANE + j
        ).start()

    abuf[z, k] = att[k]
    for step in plane_steps:
        signal(tok.at[3], z * PLANE + peer(*step))

    for load in small[4:]:
        load.wait()
    for j in range(width // LANES):
        sf[j : j + 1, :] = svm[0:1, j * LANES : (j + 1) * LANES].astype(F32)
    sblk[...] = sf[...].reshape(MSPLIT, 8, LANES).astype(BF16)
    lane = lax.broadcasted_iota(jnp.int32, (1, LANES), 1)
    s0 = jnp.full((1, LANES), route_scores[0, 0], F32)
    s1 = jnp.full((1, LANES), route_scores[0, 1], F32)
    top = jnp.maximum(s0, s1)
    e0 = jnp.exp(s0 - top)
    e1 = jnp.exp(s1 - top)
    q0 = e0 / (e0 + e1)
    q1 = e1 / (e0 + e1)
    id0 = jnp.full((1, LANES), route_ids[0, 0], jnp.int32)
    id1 = jnp.full((1, LANES), route_ids[0, 1], jnp.int32)
    meta = jnp.zeros((1, LANES), F32)
    for e in range(RESIDENT):
        w = jnp.where(id0 == e, q0, 0.0) + jnp.where(id1 == e, q1, 0.0)
        w = w.astype(BF16).astype(F32)
        picked = jnp.where((id0 == e) | (id1 == e), 1.0, 0.0)
        meta = jnp.where(lane == e, w, meta)
        meta = jnp.where(lane == RESIDENT + e, picked, meta)
    meta_out[...] = meta

    gatherer = lax.rem(z, PLANE)

    @pl.when(k != gatherer)
    def _():
        target = z * PLANE + gatherer
        copy_to(sblk, pst.at[:, k], st_send.at[0], st_recv.at[0], target).start()
        copy_to(meta_out, pme.at[k], me_send.at[0], me_recv.at[0], target).start()

    @pl.when(k == gatherer)
    def _():
        for j in range(MSPLIT):
            pst[j, k] = sblk[j]
        pme[k] = meta_out[...]

    pl.semaphore_wait(tok.at[3], PLANE - 1)
    for step in plane_steps:
        j = peer(*step)
        copy_to(
            out_weight.at[:, pl.ds(pl.multiple_of(j * bw, bw), bw)],
            wbuf.at[k],
            one_send.at[1],
            one_recv.at[1],
            z * PLANE + j,
        ).start()

    pl.semaphore_wait(tok.at[0], 2)
    for step in (2, -2):
        signal(tok.at[1], up(step) * PLANE + k)

    wait_bytes(abuf.at[0, pl.ds(0, PLANE - 1)], one_recv.at[0])
    pl.semaphore_wait(tok.at[1], 2)

    def z_copy(origin, step):
        return copy_to(
            abuf.at[origin],
            abuf.at[origin],
            one_send.at[2],
            z_recv.at[origin],
            up(step) * PLANE + k,
        )

    reach = planes // 4
    for step in range(reach, 0, -1):
        z_copy(z, step).start()
        z_copy(z, -step).start()
    for step in (reach, -reach):
        signal(tok.at[2], up(step) * PLANE + k)
    @pl.when(k == gatherer)
    def _():
        pl.semaphore_wait(tok.at[2], 2)
        wait_bytes(pst.at[pl.ds(0, PLANE - 1)], st_recv.at[0])
        wait_bytes(pme.at[pl.ds(0, PLANE - 1)], me_recv.at[0])

        def hand_on(j):
            target = j * hsplit + z

            @pl.when(target != me)
            def _():
                copy_to(pst.at[j], sbuf, st_send.at[1], st_recv.at[1], target).start()
                copy_to(pme, meta_in, me_send.at[1], me_recv.at[1], target).start()

            @pl.when(target == me)
            def _():
                sbuf[...] = pst[j]
                meta_in[...] = pme[...]

        each(MSPLIT, hand_on)

    far = up(-reach)
    wait_bytes(abuf.at[far], z_recv.at[far])
    for step in range(reach, 0, -1):
        z_copy(far, step).start()
    near = up(reach)
    wait_bytes(abuf.at[near], z_recv.at[near])
    for step in range(reach - 1, 0, -1):
        z_copy(near, -step).start()
    @pl.when(k != gatherer)
    def _():
        pl.semaphore_wait(tok.at[2], 2)

    def z_wait(i):
        origin = lax.rem(z + i, planes)

        @pl.when((origin != far) & (origin != near))
        def _():
            wait_bytes(abuf.at[origin], z_recv.at[origin])

    each(planes, z_wait, 1)

    loads[5].wait()
    wait_bytes(wbuf.at[pl.ds(0, PLANE - 1)], one_recv.at[1])

    af[...] = abuf[...].reshape(batch * 8, LANES).astype(F32)
    a = jnp.concatenate(
        [af[pl.ds(j, batch, stride=8), :] for j in range(8)], axis=1
    ).astype(BF16)
    part = nt_dot(a, wbuf[...].reshape(PLANE * wbuf.shape[1], bw))
    pbuf[...] = part.astype(BF16).reshape(hsplit, 8, part.shape[1])

    for step in patch_steps:
        j = patch_peer(step)
        copy_to(pbuf.at[j], dbuf.at[h], one_send.at[3], one_recv.at[3], m * hsplit + j).start()
    dbuf[h] = pbuf[h]

    @pl.when(z != h)
    def _():
        wait_bytes(sbuf, st_recv.at[1])
        wait_bytes(meta_in, me_recv.at[1])

    route_blk[...] = jnp.concatenate([meta_in[i] for i in range(PLANE)], axis=0)
    route_all[h] = route_blk[...]
    for step in patch_steps:
        target = m * hsplit + patch_peer(step)
        copy_to(route_blk, route_all.at[h], one_send.at[10], one_recv.at[8], target).start()
    lf[...] = sbuf[...].reshape(PLANE * 8, LANES).astype(F32)
    stream = jnp.concatenate([lf[pl.ds(c, 8, stride=8), :] for c in range(8)], axis=1)
    g8 = gainvm[pl.ds(pl.multiple_of(m * 8, 8), 8), :]
    gain_row = jnp.concatenate([g8[c : c + 1, :] for c in range(8)], axis=1)

    wait_bytes(dbuf.at[pl.ds(0, hsplit - 1)], one_recv.at[3])
    halves = []
    for half in range(hsplit // PLANE):
        part_sum = dbuf[half * PLANE].astype(F32)
        for j in range(1, PLANE):
            part_sum = part_sum + dbuf[half * PLANE + j].astype(F32)
        halves.append(part_sum)
    proj = jnp.concatenate(halves, axis=1).astype(BF16).astype(F32)
    resid = stream + proj
    resid_ref[...] = resid
    yblk[...] = (resid * gain_row).astype(BF16)
    xbuf[h] = yblk[...]
    for step in patch_steps:
        target = m * hsplit + patch_peer(step)
        copy_to(yblk, xbuf.at[h], one_send.at[5], one_recv.at[5], target).start()
    ssq = jnp.sum(resid * resid, axis=1, keepdims=True)
    meta_blk[...] = jnp.broadcast_to(ssq, (8, LANES))
    meta_all[h] = meta_blk[...]
    for step in patch_steps:
        target = m * hsplit + patch_peer(step)
        copy_to(meta_blk, meta_all.at[h], one_send.at[4], one_recv.at[4], target).start()

    wait_bytes(route_all.at[pl.ds(0, hsplit - 1)], one_recv.at[8])
    info = route_all[...].reshape(batch, LANES)
    info_t = info.T
    ia = lax.broadcasted_iota(jnp.int32, (batch, batch), 0)
    ib = lax.broadcasted_iota(jnp.int32, (batch, batch), 1)
    before_t = jnp.where(ia < ib, 1.0, 0.0).astype(BF16)
    before = jnp.where(ib < ia, 1.0, 0.0).astype(BF16)
    ranks_t = nn_dot(info_t[0:8].astype(BF16), before_t)
    ranks = nn_dot(before, info.astype(BF16))

    def place_of(rank, picked):
        out = rank
        for c in range(1, quarters):
            step = float(c * pad - edges[c] - (c - 1) * pad + edges[c - 1])
            if step:
                out = out + jnp.where(rank >= float(edges[c]), step, 0.0)
        return jnp.where(picked > 0.5, out, -1.0)

    rows_i = [place_of(ranks_t[RESIDENT + e : RESIDENT + e + 1], info_t[RESIDENT + e : RESIDENT + e + 1]) for e in range(RESIDENT)]
    cols_i = [place_of(ranks[:, RESIDENT + e : RESIDENT + e + 1], info[:, RESIDENT + e : RESIDENT + e + 1]) for e in range(RESIDENT)]
    wait_bytes(xbuf.at[pl.ds(0, hsplit - 1)], one_recv.at[5])
    x = xbuf[...].reshape(batch, bw)
    r_iota = lax.broadcasted_iota(jnp.int32, (rows, batch), 0).astype(F32)
    for e in range(RESIDENT):
        pick = jnp.where(r_iota == rows_i[e], 1.0, 0.0).astype(BF16)
        xcs[e] = nn_dot(pick, x).astype(BF16)
    loads[2].wait()
    loads[3].wait()

    fwd = MSPLIT // 2
    bwd = MSPLIT - 1 - fwd

    def ring(q, step):
        turn = sgn * (1 - 2 * (q // fwd))
        return lax.rem(m + turn * step + 2 * MSPLIT, MSPLIT)

    def ring_dev(q, step):
        return ring(q, step) * hsplit + low

    def sized(chunk, body):
        odd = lax.rem(chunk, 2)

        @pl.when(odd == 0)
        def _():
            body(pl.ds(0, pad), 0)

        @pl.when(odd == 1)
        def _():
            body(pl.ds(0, short), 1)

    def rs_start(slot, q, chunk, target):
        def go(r, kind):
            copy_to(
                rs_send.at[slot, q, r],
                rs_recv.at[slot, q, r],
                size_send.at[kind],
                rs_sem.at[slot, q],
                target,
            ).start()

        sized(chunk, go)

    def rs_wait(slot, q, chunk):
        sized(chunk, lambda r, kind: wait_bytes(rs_recv.at[slot, q, r], rs_sem.at[slot, q]))

    def first(q):
        cols = pl.ds(pl.multiple_of(q * LANES, LANES), LANES)
        for e in range(RESIDENT):
            rhs = jnp.concatenate([gbuf[e, :, cols], ubuf[e, :, cols]], axis=1)
            r = nn_dot(xcs[e], rhs)
            own[q, e * quarters : (e + 1) * quarters] = r.reshape(quarters, pad, 2 * LANES)
        rs_send[0, q] = own[q, ring(q, fwd)].astype(BF16)
        rs_start(0, q, ring(q, fwd), ring_dev(q, 1))
        rs_send[fwd, q] = own[q, ring(q, -bwd)].astype(BF16)
        rs_start(fwd, q, ring(q, -bwd), ring_dev(q, -1))

    each(pieces, first)

    wait_bytes(meta_all.at[pl.ds(0, hsplit - 1)], one_recv.at[4])
    ssq_row[...] = meta_all[...].reshape(batch, LANES).T[0:1]
    ssq_all[m] = ssq_row[...]

    def ssq_send(i):
        j = lax.rem(m + i, MSPLIT)
        copy_to(ssq_row, ssq_all.at[m], one_send.at[6], one_recv.at[6], j * hsplit + low).start()

    each(MSPLIT, ssq_send, 1)

    for t in range(1, fwd):

        def onward(q, t=t):
            chunk = ring(q, fwd - t)
            rs_wait(t - 1, q, chunk)
            v = rs_recv[t - 1, q].astype(F32) + own[q, chunk]
            rs_send[t, q] = v.astype(BF16)
            rs_start(t, q, chunk, ring_dev(q, 1))
            if t < bwd:
                b = fwd + t
                chunk = ring(q, t - bwd)
                rs_wait(b - 1, q, chunk)
                v = rs_recv[b - 1, q].astype(F32) + own[q, chunk]
                rs_send[b, q] = v.astype(BF16)
                rs_start(b, q, chunk, ring_dev(q, -1))

        each(pieces, onward)

    wait_bytes(ssq_all.at[pl.ds(0, MSPLIT - 1)], one_recv.at[6])
    power = ssq_all[0]
    for j in range(1, MSPLIT):
        power = power + ssq_all[j]
    chunk_row = jnp.where(m < quarters, rows_i[0], rows_i[1])
    c_iota = lax.broadcasted_iota(jnp.int32, (pad, batch), 0) + lax.rem(m, quarters) * pad
    hit = c_iota.astype(F32) == chunk_row
    mean = jnp.sum(jnp.where(hit, power, 0.0), axis=1, keepdims=True) / float(width)
    factor = lax.rsqrt(mean + 1e-05)

    legs = (1, 2, 3, 4, -1, -2, -3)

    def ag_start(leg, q, chunk, step):
        def go(r, kind):
            copy_to(
                hbuf.at[q, chunk, r],
                hbuf.at[q, chunk, r],
                size_send.at[2 + kind],
                ag_sem.at[legs.index(leg), q],
                ring_dev(q, step),
            ).start()

        sized(chunk, go)

    def ag_wait(leg, q):
        chunk = ring(q, -leg)
        sized(chunk, lambda r, kind: wait_bytes(hbuf.at[q, chunk, r], ag_sem.at[legs.index(leg), q]))

    def finish(q):
        rs_wait(fwd - 1, q, m)
        rs_wait(MSPLIT - 2, q, m)
        v = own[q, m] + rs_recv[fwd - 1, q].astype(F32) + rs_recv[MSPLIT - 2, q].astype(F32)
        v = v * factor
        ga = v[:, :LANES]
        up_half = v[:, LANES:]
        hbuf[q, m] = (ga / (1.0 + jnp.exp(-ga)) * up_half).astype(BF16)
        for leg in (2, -2, 1, -1):
            ag_start(leg, q, m, leg)

    each(pieces, finish)

    def relay(q):
        ag_wait(2, q)
        ag_start(4, q, ring(q, -2), 2)
        ag_start(3, q, ring(q, -2), 1)
        ag_wait(-2, q)
        ag_start(-3, q, ring(q, 2), -1)

    each(pieces, relay)

    loads[4].wait()
    col_iota = lax.broadcasted_iota(jnp.int32, (batch, rows), 1).astype(F32)
    row_iota = lax.broadcasted_iota(jnp.int32, (rows, LANES), 0)
    filled = lax.rem(row_iota, 2 * pad) < pad + short
    for e in range(RESIDENT):
        picks[e] = jnp.where(col_iota == cols_i[e], 1.0, 0.0).astype(BF16)
    acc[...] = jnp.zeros_like(acc)

    def down(q):
        for leg in (1, -1, 3, -3, 4):
            ag_wait(leg, q)
        units = pl.ds(pl.multiple_of(q * LANES, LANES), LANES)
        for e in range(RESIDENT):
            hc = hbuf[q, e * quarters : (e + 1) * quarters].astype(F32).reshape(rows, LANES)
            hc = jnp.where(filled, hc, 0.0).astype(BF16)
            spread = nn_dot(picks[e], hc).astype(BF16)
            acc[e] += nn_dot(spread, dwbuf[e, units, :])

    each(pieces, down)
    total = info[:, 0:1] * acc[0]
    for e in range(1, RESIDENT):
        total = total + info[:, e : e + 1] * acc[e]
    kout[...] = total.astype(BF16).reshape(hsplit, 8, bw)

    for step in patch_steps:
        j = patch_peer(step)
        copy_to(kout.at[j], kin.at[h], one_send.at[9], one_recv.at[7], m * hsplit + j).start()
    kin[h] = kout[h]
    wait_bytes(kin.at[pl.ds(0, hsplit - 1)], one_recv.at[7])
    ffn = kin[0].astype(F32)
    for j in range(1, hsplit):
        ffn = ffn + kin[j].astype(F32)
    final = resid_ref[...] + ffn
    for c in range(8):
        lf[pl.ds(c, 8, stride=8), :] = final[:, c * LANES : (c + 1) * LANES]
    lout[...] = lf[...].reshape(PLANE, 8, LANES).astype(BF16)

    def row_send(i):
        target = h * PLANE + i

        @pl.when(target != me)
        def _():
            copy_to(lout.at[i], lbuf.at[m], l_send.at[i], l_recv.at[m], target).start()

    each(PLANE, row_send)

    @pl.when(z == h)
    def _():
        lbuf[m] = lout[k]

    wait_bytes(abuf.at[0, pl.ds(0, PLANE - 1)], one_send.at[0])
    wait_bytes(wbuf.at[pl.ds(0, PLANE - 1)], one_send.at[1])
    wait_bytes(abuf.at[pl.ds(0, planes - 1)], one_send.at[2])
    wait_bytes(dbuf.at[pl.ds(0, hsplit - 1)], one_send.at[3])
    wait_bytes(meta_all.at[pl.ds(0, hsplit - 1)], one_send.at[4])
    wait_bytes(xbuf.at[pl.ds(0, hsplit - 1)], one_send.at[5])
    wait_bytes(ssq_all.at[pl.ds(0, MSPLIT - 1)], one_send.at[6])
    for parity in range(2):

        @pl.when(lax.rem(m, 2) == parity)
        def _(parity=parity):
            rs_even = MSPLIT // 2 - (1 - parity)
            ag_steps = (0, 0, 0, 0, -2, -2, 2)
            ag_even = sum((parity + step) % 2 == 0 for step in ag_steps)
            wait_bytes(rs_send.at[pl.ds(0, rs_even)], size_send.at[0])
            wait_bytes(rs_send.at[pl.ds(0, hops - rs_even), :, pl.ds(0, short)], size_send.at[1])
            wait_bytes(hbuf.at[:, pl.ds(0, ag_even)], size_send.at[2])
            wait_bytes(hbuf.at[:, pl.ds(0, hops - ag_even), pl.ds(0, short)], size_send.at[3])

    wait_bytes(kin.at[pl.ds(0, hsplit - 1)], one_send.at[9])
    wait_bytes(route_all.at[pl.ds(0, hsplit - 1)], one_send.at[10])

    @pl.when(k != gatherer)
    def _():
        wait_bytes(sblk, st_send.at[0])
        wait_bytes(meta_out, me_send.at[0])

    @pl.when((k == gatherer) & (z == h))
    def _():
        wait_bytes(pst.at[pl.ds(0, MSPLIT - 1)], st_send.at[1])
        wait_bytes(route_all.at[pl.ds(0, MSPLIT - 1)], me_send.at[1])

    @pl.when((k == gatherer) & (z != h))
    def _():
        wait_bytes(pst, st_send.at[1])
        wait_bytes(route_all.at[pl.ds(0, MSPLIT)], me_send.at[1])

    def drain(j):
        @pl.when(j * hsplit + z != me)
        def _():
            wait_bytes(lbuf.at[j], l_recv.at[j])

        @pl.when(h * PLANE + j != me)
        def _():
            wait_bytes(lout.at[j], l_send.at[j])

    each(MSPLIT, drain)

    qf[...] = lbuf[...].reshape(MSPLIT * 8, LANES).astype(F32)
    for j in range(width // LANES):
        out_ref[0:1, j * LANES : (j + 1) * LANES] = qf[j : j + 1, :]


def on_device(
    stream_in,
    query,
    key_new,
    value_new,
    key_cache,
    value_cache,
    lengths,
    route_ids,
    route_scores,
    out_weight,
    norm_gain,
    gate_weight,
    up_weight,
    down_weight,
):
    n = lax.axis_size("gx")
    width = stream_in.shape[1]
    slots = key_cache.shape[1]
    kv = key_cache.shape[2]
    hidden = gate_weight.shape[2]
    bw = width // MSPLIT
    hsplit = n // MSPLIT
    planes = n // PLANE
    cols = out_weight.shape[1]
    quarters = MSPLIT // RESIDENT
    cap = 5 * n // 8
    edges = [-(-(cap * c // quarters) // 8) * 8 for c in range(quarters + 1)]
    pad = edges[1] - edges[0]
    short = edges[2] - edges[1]
    assert [b - a for a, b in zip(edges, edges[1:])] == [pad, short] * (quarters // 2)
    pieces = hidden // LANES
    cfg = dict(n=n, width=width, hidden=hidden, edges=edges, pad=pad, short=short)
    hops = MSPLIT - 1

    def vmem(*shape, dtype=BF16):
        return pltpu.VMEM(shape, dtype)

    scratch = [
        vmem(slots, kv),
        vmem(slots, kv),
        vmem(*gate_weight.shape),
        vmem(*up_weight.shape),
        vmem(*down_weight.shape),
        vmem(PLANE, cols, bw),
        vmem(width // LANES, LANES, dtype=F32),
        vmem(width // LANES, LANES, dtype=F32),
        vmem(MSPLIT, 8, LANES),
        vmem(KVH, 8, HS),
        vmem(planes, PLANE, 8, HS),
        vmem(n * 8, LANES, dtype=F32),
        vmem(hsplit, 8, PLANE * cols),
        vmem(hsplit, 8, PLANE * cols),
        vmem(PLANE, 8, LANES),
        vmem(1, LANES, dtype=F32),
        vmem(PLANE, 1, LANES, dtype=F32),
        vmem(8, LANES, dtype=F32),
        vmem(hsplit, 8, LANES, dtype=F32),
        vmem(8, bw, dtype=F32),
        vmem(8, bw),
        vmem(hsplit, 8, bw),
        vmem(1, LANES, dtype=F32),
        vmem(MSPLIT, 1, LANES, dtype=F32),
        vmem(RESIDENT, quarters * pad, bw),
        vmem(pieces, MSPLIT, pad, 2 * LANES, dtype=F32),
        vmem(hops, pieces, pad, 2 * LANES),
        vmem(hops, pieces, pad, 2 * LANES),
        vmem(pieces, MSPLIT, pad, LANES),
        vmem(hsplit, 8, bw),
        vmem(hsplit, 8, bw),
        vmem(PLANE * 8, LANES, dtype=F32),
        vmem(PLANE, 8, LANES),
        vmem(MSPLIT, 8, LANES),
        vmem(1, width),
        vmem(1, width),
        vmem(1, kv),
        vmem(1, kv),
        vmem(width // LANES, LANES, dtype=F32),
        pltpu.SMEM((1,), jnp.int32),
        pltpu.SMEM((1, 2), jnp.int32),
        pltpu.SMEM((1, 2), F32),
        vmem(MSPLIT, PLANE, 8, LANES),
        vmem(PLANE, 1, LANES, dtype=F32),
        vmem(8, LANES, dtype=F32),
        vmem(hsplit, 8, LANES, dtype=F32),
        vmem(RESIDENT, n, bw, dtype=F32),
        vmem(RESIDENT, n, quarters * pad),
        pltpu.SemaphoreType.DMA((14,)),
        pltpu.SemaphoreType.DMA((11,)),
        pltpu.SemaphoreType.DMA((9,)),
        pltpu.SemaphoreType.DMA((planes,)),
        pltpu.SemaphoreType.REGULAR((4,)),
        pltpu.SemaphoreType.DMA((4,)),
        pltpu.SemaphoreType.DMA((2,)),
        pltpu.SemaphoreType.DMA((2,)),
        pltpu.SemaphoreType.DMA((2,)),
        pltpu.SemaphoreType.DMA((2,)),
        pltpu.SemaphoreType.DMA((hops, pieces)),
        pltpu.SemaphoreType.DMA((hops, pieces)),
        pltpu.SemaphoreType.DMA((PLANE,)),
        pltpu.SemaphoreType.DMA((MSPLIT,)),
    ]
    local = pl.BlockSpec(memory_space=pltpu.VMEM)
    anywhere = pl.BlockSpec(memory_space=pl.ANY)
    return pl.pallas_call(
        functools.partial(layer_kernel, cfg),
        out_shape=jax.ShapeDtypeStruct((1, width), F32),
        in_specs=[anywhere] * 14,
        out_specs=local,
        scratch_shapes=scratch,
        compiler_params=pltpu.CompilerParams(
            collective_id=0, has_side_effects=True, vmem_limit_bytes=60 * 1024 * 1024
        ),
        name="layer",
    )(
        lengths,
        route_ids,
        route_scores,
        stream_in,
        query,
        key_new,
        value_new,
        norm_gain.reshape(width // LANES, LANES),
        key_cache.reshape(slots, kv),
        value_cache.reshape(slots, kv),
        out_weight.T,
        gate_weight,
        up_weight,
        down_weight,
    ).astype(BF16)


def solution(mesh):
    rows = P(("groups", "gx"), None)
    in_specs = (
        rows,
        rows,
        rows,
        rows,
        P(("groups", "gx"), None, None),
        P(("groups", "gx"), None, None),
        P(("groups", "gx")),
        rows,
        rows,
        P(None, "gx"),
        P(),
        P(None, "gx", None),
        P(None, "gx", None),
        P(None, "gx", None),
    )
    return jax.shard_map(
        on_device, mesh=mesh, in_specs=in_specs, out_specs=rows, check_vma=False
    )
```

```python
import functools

import jax
import jax.numpy as jnp
from jax import lax
from jax.experimental import pallas as pl
from jax.experimental.pallas import tpu as pltpu
from jax.sharding import PartitionSpec as P

NH = 64
KVH = 8
HS = 128
RESIDENT = 2
MSPLIT = 8
PLANE = 8
LANES = 128
BF16 = jnp.bfloat16
F32 = jnp.float32
MESH = pl.DeviceIdType.MESH


def nt_dot(a, b):
    return lax.dot_general(a, b, (((1,), (1,)), ((), ())), preferred_element_type=F32)


def nn_dot(a, b):
    return lax.dot_general(a, b, (((1,), (0,)), ((), ())), preferred_element_type=F32)


def copy_to(src, dst, send, recv, target):
    return pltpu.make_async_remote_copy(
        src_ref=src,
        dst_ref=dst,
        send_sem=send,
        recv_sem=recv,
        device_id={"gx": target},
        device_id_type=MESH,
    )


def wait_bytes(ref, sem):
    pltpu.make_async_copy(ref, ref, sem).wait()


def each(count, body, start=0):
    def step(i, carry):
        body(i)
        return carry

    lax.fori_loop(start, count, step, 0)


def layer_kernel(
    cfg,
    lengths_in,
    ids_in,
    scores_in,
    stream_in,
    query,
    key_new,
    value_new,
    gain,
    key_cache,
    value_cache,
    out_weight,
    gate_weight,
    up_weight,
    down_weight,
    out_ref,
    kbuf,
    vbuf,
    gbuf,
    ubuf,
    dwbuf,
    wbuf,
    qf,
    sf,
    sblk,
    att,
    abuf,
    af,
    pbuf,
    dbuf,
    sbuf,
    meta_out,
    meta_in,
    meta_blk,
    meta_all,
    resid_ref,
    yblk,
    xbuf,
    ssq_row,
    ssq_all,
    xcs,
    own,
    rs_send,
    rs_recv,
    hbuf,
    kout,
    kin,
    lf,
    lout,
    lbuf,
    svm,
    qvm,
    knvm,
    vnvm,
    gainvm,
    lengths,
    route_ids,
    route_scores,
    pst,
    pme,
    route_blk,
    route_all,
    acc,
    picks,
    wvm,
    loc_sem,
    one_send,
    one_recv,
    z_recv,
    tok,
    size_send,
    st_send,
    st_recv,
    me_send,
    me_recv,
    rs_sem,
    ag_sem,
    l_send,
    l_recv,
):
    n = cfg["n"]
    hsplit = n // MSPLIT
    planes = n // PLANE
    batch = n
    width = cfg["width"]
    bw = width // MSPLIT
    pieces = cfg["hidden"] // LANES
    edges = cfg["edges"]
    pad = cfg["pad"]
    short = cfg["short"]
    quarters = MSPLIT // RESIDENT
    rows = quarters * pad
    hops = MSPLIT - 1

    me = lax.axis_index("gx")
    z = me // PLANE
    k = lax.rem(me, PLANE)
    m = me // hsplit
    h = lax.rem(me, hsplit)
    low = me - m * hsplit
    sgn = 1 - 2 * lax.rem(me, 2)

    def up(step):
        return lax.rem(z + sgn * step + 2 * planes, planes)

    def signal(sem, target):
        pl.semaphore_signal(sem, inc=1, device_id={"gx": target}, device_id_type=MESH)

    small = [
        pltpu.make_async_copy(src, dst, loc_sem.at[6 + i])
        for i, (src, dst) in enumerate(
            [
                (query, qvm),
                (key_new, knvm),
                (value_new, vnvm),
                (lengths_in, lengths),
                (stream_in, svm),
                (gain, gainvm),
                (ids_in, route_ids),
                (scores_in, route_scores),
            ]
        )
    ]
    for load in small:
        load.start()
    loads = [
        pltpu.make_async_copy(key_cache, kbuf, loc_sem.at[0]),
        pltpu.make_async_copy(value_cache, vbuf, loc_sem.at[1]),
        pltpu.make_async_copy(gate_weight, gbuf, loc_sem.at[2]),
        pltpu.make_async_copy(up_weight, ubuf, loc_sem.at[3]),
        pltpu.make_async_copy(down_weight, dwbuf, loc_sem.at[4]),
        pltpu.make_async_copy(out_weight, wvm, loc_sem.at[5]),
    ]
    for load in loads[:2]:
        load.start()

    xs = k // 2
    core = lax.rem(k, 2)

    def peer(dx, dc):
        return 2 * lax.rem(xs + dx, PLANE // 2) + lax.rem(core + dc, 2)

    plane_steps = [(dx, dc) for dx in (2, 3, 1) for dc in (0, 1)] + [(0, 1)]
    patch_steps = [(dz, dx, dc) for dx in (2, 3, 1) for dz in (1, 0) for dc in (0, 1)]
    patch_steps += [(1, 0, 0), (1, 0, 1), (0, 0, 1)]

    def patch_peer(step):
        dz, dx, dc = step
        return lax.rem(h // PLANE + dz, 2) * PLANE + peer(dx, dc)

    barrier = pltpu.get_barrier_semaphore()

    for step in (1, -1):
        signal(barrier, up(step) * PLANE + k)

    def greet(i):
        signal(barrier, z * PLANE + lax.rem(k + i, PLANE))

    each(PLANE, greet, 1)

    loads[5].start()
    for load in loads[2:5]:
        load.start()

    for load in small[:4]:
        load.wait()
    for j in range(width // LANES):
        qf[j : j + 1, :] = qvm[0:1, j * LANES : (j + 1) * LANES].astype(F32)

    def per_group(row_ref):
        return jnp.concatenate(
            [
                jnp.broadcast_to(row_ref[0:1, g * HS : (g + 1) * HS].astype(F32), (NH // KVH, HS))
                for g in range(KVH)
            ],
            axis=0,
        )

    q_all = qf[...]
    scale = HS ** (-0.5)
    o = jnp.sum(q_all * per_group(knvm), axis=1, keepdims=True) * scale
    v_own = per_group(vnvm)
    loads[0].wait()
    slots = kbuf.shape[0]
    s = jnp.concatenate(
        [
            nt_dot(q_all[g * 8 : (g + 1) * 8].astype(BF16), kbuf[:, g * HS : (g + 1) * HS])
            for g in range(KVH)
        ],
        axis=0,
    )
    live = lax.broadcasted_iota(jnp.int32, (NH, slots), 1) < lengths[0]
    s = jnp.where(live, s * scale, -1e30)
    t = jnp.maximum(jnp.max(s, axis=1, keepdims=True), o)
    es = jnp.exp(s - t)
    eo = jnp.exp(o - t)
    total = jnp.sum(es, axis=1, keepdims=True) + eo
    p = es / total
    own_term = (eo / total).astype(BF16).astype(F32) * v_own
    loads[1].wait()
    for g in range(KVH):
        r = slice(g * 8, (g + 1) * 8)
        mixed = nn_dot(p[r].astype(BF16), vbuf[:, g * HS : (g + 1) * HS])
        att[g] = (mixed + own_term[r]).astype(BF16)

    pl.semaphore_wait(barrier, PLANE + 1)
    for step in (1, -1):
        signal(tok.at[0], up(step) * PLANE + k)

    for step in plane_steps:
        j = peer(*step)
        copy_to(
            att.at[j], abuf.at[z, k], one_send.at[0], one_recv.at[0], z * PLANE + j
        ).start()

    abuf[z, k] = att[k]
    for step in plane_steps:
        signal(tok.at[3], z * PLANE + peer(*step))

    for load in small[4:]:
        load.wait()
    for j in range(width // LANES):
        sf[j : j + 1, :] = svm[0:1, j * LANES : (j + 1) * LANES].astype(F32)
    sblk[...] = sf[...].reshape(MSPLIT, 8, LANES).astype(BF16)
    lane = lax.broadcasted_iota(jnp.int32, (1, LANES), 1)
    s0 = jnp.full((1, LANES), route_scores[0, 0], F32)
    s1 = jnp.full((1, LANES), route_scores[0, 1], F32)
    top = jnp.maximum(s0, s1)
    e0 = jnp.exp(s0 - top)
    e1 = jnp.exp(s1 - top)
    q0 = e0 / (e0 + e1)
    q1 = e1 / (e0 + e1)
    id0 = jnp.full((1, LANES), route_ids[0, 0], jnp.int32)
    id1 = jnp.full((1, LANES), route_ids[0, 1], jnp.int32)
    meta = jnp.zeros((1, LANES), F32)
    for e in range(RESIDENT):
        w = jnp.where(id0 == e, q0, 0.0) + jnp.where(id1 == e, q1, 0.0)
        w = w.astype(BF16).astype(F32)
        picked = jnp.where((id0 == e) | (id1 == e), 1.0, 0.0)
        meta = jnp.where(lane == e, w, meta)
        meta = jnp.where(lane == RESIDENT + e, picked, meta)
    meta_out[...] = meta

    gatherer = lax.rem(z, PLANE)

    @pl.when(k != gatherer)
    def _():
        target = z * PLANE + gatherer
        copy_to(sblk, pst.at[:, k], st_send.at[0], st_recv.at[0], target).start()
        copy_to(meta_out, pme.at[k], me_send.at[0], me_recv.at[0], target).start()

    @pl.when(k == gatherer)
    def _():
        for j in range(MSPLIT):
            pst[j, k] = sblk[j]
        pme[k] = meta_out[...]

    loads[5].wait()
    pl.semaphore_wait(tok.at[3], PLANE - 1)
    for step in sorted(plane_steps, key=lambda step: step[0] == 2):
        j = peer(*step)
        copy_to(
            wvm.at[:, pl.ds(pl.multiple_of(j * bw, bw), bw)],
            wbuf.at[k],
            one_send.at[1],
            one_recv.at[1],
            z * PLANE + j,
        ).start()

    pl.semaphore_wait(tok.at[0], 2)
    for step in (2, -2):
        signal(tok.at[1], up(step) * PLANE + k)

    wait_bytes(abuf.at[0, pl.ds(0, PLANE - 1)], one_recv.at[0])
    pl.semaphore_wait(tok.at[1], 2)

    def z_copy(origin, step):
        return copy_to(
            abuf.at[origin],
            abuf.at[origin],
            one_send.at[2],
            z_recv.at[origin],
            up(step) * PLANE + k,
        )

    reach = planes // 4
    for step in range(reach, 0, -1):
        z_copy(z, step).start()
        z_copy(z, -step).start()
    for step in (reach, -reach):
        signal(tok.at[2], up(step) * PLANE + k)
    @pl.when(k == gatherer)
    def _():
        pl.semaphore_wait(tok.at[2], 2)
        wait_bytes(pst.at[pl.ds(0, PLANE - 1)], st_recv.at[0])
        wait_bytes(pme.at[pl.ds(0, PLANE - 1)], me_recv.at[0])

        def hand_on(j):
            target = j * hsplit + z

            @pl.when(target != me)
            def _():
                copy_to(pst.at[j], sbuf, st_send.at[1], st_recv.at[1], target).start()
                copy_to(pme, meta_in, me_send.at[1], me_recv.at[1], target).start()

            @pl.when(target == me)
            def _():
                sbuf[...] = pst[j]
                meta_in[...] = pme[...]

        each(MSPLIT, hand_on)

    far = up(-reach)
    wait_bytes(abuf.at[far], z_recv.at[far])
    for step in range(reach, 0, -1):
        z_copy(far, step).start()
    near = up(reach)
    wait_bytes(abuf.at[near], z_recv.at[near])
    for step in range(reach - 1, 0, -1):
        z_copy(near, -step).start()
    @pl.when(k != gatherer)
    def _():
        pl.semaphore_wait(tok.at[2], 2)

    def z_wait(i):
        origin = lax.rem(z + i, planes)

        @pl.when((origin != far) & (origin != near))
        def _():
            wait_bytes(abuf.at[origin], z_recv.at[origin])

    each(planes, z_wait, 1)

    wbuf[k] = wvm[:, pl.ds(pl.multiple_of(k * bw, bw), bw)]
    wait_bytes(wbuf.at[pl.ds(0, PLANE - 1)], one_recv.at[1])

    af[...] = abuf[...].reshape(batch * 8, LANES).astype(F32)
    a = jnp.concatenate(
        [af[pl.ds(j, batch, stride=8), :] for j in range(8)], axis=1
    ).astype(BF16)
    part = nt_dot(a, wbuf[...].reshape(PLANE * wbuf.shape[1], bw))
    pbuf[...] = part.astype(BF16).reshape(hsplit, 8, part.shape[1])

    for step in patch_steps:
        j = patch_peer(step)
        copy_to(pbuf.at[j], dbuf.at[h], one_send.at[3], one_recv.at[3], m * hsplit + j).start()
    dbuf[h] = pbuf[h]

    @pl.when(z != h)
    def _():
        wait_bytes(sbuf, st_recv.at[1])
        wait_bytes(meta_in, me_recv.at[1])

    route_blk[...] = jnp.concatenate([meta_in[i] for i in range(PLANE)], axis=0)
    route_all[h] = route_blk[...]
    for step in patch_steps:
        target = m * hsplit + patch_peer(step)
        copy_to(route_blk, route_all.at[h], one_send.at[10], one_recv.at[8], target).start()
    lf[...] = sbuf[...].reshape(PLANE * 8, LANES).astype(F32)
    stream = jnp.concatenate([lf[pl.ds(c, 8, stride=8), :] for c in range(8)], axis=1)
    g8 = gainvm[pl.ds(pl.multiple_of(m * 8, 8), 8), :]
    gain_row = jnp.concatenate([g8[c : c + 1, :] for c in range(8)], axis=1)

    wait_bytes(dbuf.at[pl.ds(0, hsplit - 1)], one_recv.at[3])
    halves = []
    for half in range(hsplit // PLANE):
        part_sum = dbuf[half * PLANE].astype(F32)
        for j in range(1, PLANE):
            part_sum = part_sum + dbuf[half * PLANE + j].astype(F32)
        halves.append(part_sum)
    proj = jnp.concatenate(halves, axis=1).astype(BF16).astype(F32)
    resid = stream + proj
    resid_ref[...] = resid
    yblk[...] = (resid * gain_row).astype(BF16)
    xbuf[h] = yblk[...]
    for step in patch_steps:
        target = m * hsplit + patch_peer(step)
        copy_to(yblk, xbuf.at[h], one_send.at[5], one_recv.at[5], target).start()
    ssq = jnp.sum(resid * resid, axis=1, keepdims=True)
    meta_blk[...] = jnp.broadcast_to(ssq, (8, LANES))
    meta_all[h] = meta_blk[...]
    for step in patch_steps:
        target = m * hsplit + patch_peer(step)
        copy_to(meta_blk, meta_all.at[h], one_send.at[4], one_recv.at[4], target).start()

    wait_bytes(route_all.at[pl.ds(0, hsplit - 1)], one_recv.at[8])
    info = route_all[...].reshape(batch, LANES)
    info_t = info.T
    ia = lax.broadcasted_iota(jnp.int32, (batch, batch), 0)
    ib = lax.broadcasted_iota(jnp.int32, (batch, batch), 1)
    before_t = jnp.where(ia < ib, 1.0, 0.0).astype(BF16)
    before = jnp.where(ib < ia, 1.0, 0.0).astype(BF16)
    ranks_t = nn_dot(info_t[0:8].astype(BF16), before_t)
    ranks = nn_dot(before, info.astype(BF16))

    def place_of(rank, picked):
        out = rank
        for c in range(1, quarters):
            step = float(c * pad - edges[c] - (c - 1) * pad + edges[c - 1])
            if step:
                out = out + jnp.where(rank >= float(edges[c]), step, 0.0)
        return jnp.where(picked > 0.5, out, -1.0)

    rows_i = [place_of(ranks_t[RESIDENT + e : RESIDENT + e + 1], info_t[RESIDENT + e : RESIDENT + e + 1]) for e in range(RESIDENT)]
    cols_i = [place_of(ranks[:, RESIDENT + e : RESIDENT + e + 1], info[:, RESIDENT + e : RESIDENT + e + 1]) for e in range(RESIDENT)]
    wait_bytes(xbuf.at[pl.ds(0, hsplit - 1)], one_recv.at[5])
    x = xbuf[...].reshape(batch, bw)
    r_iota = lax.broadcasted_iota(jnp.int32, (rows, batch), 0).astype(F32)
    for e in range(RESIDENT):
        pick = jnp.where(r_iota == rows_i[e], 1.0, 0.0).astype(BF16)
        xcs[e] = nn_dot(pick, x).astype(BF16)
    loads[2].wait()
    loads[3].wait()

    fwd = MSPLIT // 2
    bwd = MSPLIT - 1 - fwd

    def ring(q, step):
        turn = sgn * (1 - 2 * (q // fwd))
        return lax.rem(m + turn * step + 2 * MSPLIT, MSPLIT)

    def ring_dev(q, step):
        return ring(q, step) * hsplit + low

    def sized(chunk, body):
        odd = lax.rem(chunk, 2)

        @pl.when(odd == 0)
        def _():
            body(pl.ds(0, pad), 0)

        @pl.when(odd == 1)
        def _():
            body(pl.ds(0, short), 1)

    def rs_start(slot, q, chunk, target):
        def go(r, kind):
            copy_to(
                rs_send.at[slot, q, r],
                rs_recv.at[slot, q, r],
                size_send.at[kind],
                rs_sem.at[slot, q],
                target,
            ).start()

        sized(chunk, go)

    def rs_wait(slot, q, chunk):
        sized(chunk, lambda r, kind: wait_bytes(rs_recv.at[slot, q, r], rs_sem.at[slot, q]))

    def first(q):
        cols = pl.ds(pl.multiple_of(q * LANES, LANES), LANES)
        for e in range(RESIDENT):
            rhs = jnp.concatenate([gbuf[e, :, cols], ubuf[e, :, cols]], axis=1)
            r = nn_dot(xcs[e], rhs)
            own[q, e * quarters : (e + 1) * quarters] = r.reshape(quarters, pad, 2 * LANES)
        rs_send[0, q] = own[q, ring(q, fwd)].astype(BF16)
        rs_start(0, q, ring(q, fwd), ring_dev(q, 1))
        rs_send[fwd, q] = own[q, ring(q, -bwd)].astype(BF16)
        rs_start(fwd, q, ring(q, -bwd), ring_dev(q, -1))

    each(pieces, first)

    wait_bytes(meta_all.at[pl.ds(0, hsplit - 1)], one_recv.at[4])
    ssq_row[...] = meta_all[...].reshape(batch, LANES).T[0:1]
    ssq_all[m] = ssq_row[...]

    def ssq_send(i):
        j = lax.rem(m + i, MSPLIT)
        copy_to(ssq_row, ssq_all.at[m], one_send.at[6], one_recv.at[6], j * hsplit + low).start()

    each(MSPLIT, ssq_send, 1)

    for t in range(1, fwd):

        def onward(q, t=t):
            chunk = ring(q, fwd - t)
            rs_wait(t - 1, q, chunk)
            v = rs_recv[t - 1, q].astype(F32) + own[q, chunk]
            rs_send[t, q] = v.astype(BF16)
            rs_start(t, q, chunk, ring_dev(q, 1))
            if t < bwd:
                b = fwd + t
                chunk = ring(q, t - bwd)
                rs_wait(b - 1, q, chunk)
                v = rs_recv[b - 1, q].astype(F32) + own[q, chunk]
                rs_send[b, q] = v.astype(BF16)
                rs_start(b, q, chunk, ring_dev(q, -1))

        each(pieces, onward)

    wait_bytes(ssq_all.at[pl.ds(0, MSPLIT - 1)], one_recv.at[6])
    power = ssq_all[0]
    for j in range(1, MSPLIT):
        power = power + ssq_all[j]
    chunk_row = jnp.where(m < quarters, rows_i[0], rows_i[1])
    c_iota = lax.broadcasted_iota(jnp.int32, (pad, batch), 0) + lax.rem(m, quarters) * pad
    hit = c_iota.astype(F32) == chunk_row
    mean = jnp.sum(jnp.where(hit, power, 0.0), axis=1, keepdims=True) / float(width)
    factor = lax.rsqrt(mean + 1e-05)

    legs = (1, 2, 3, 4, -1, -2, -3)

    def ag_start(leg, q, chunk, step):
        def go(r, kind):
            copy_to(
                hbuf.at[q, chunk, r],
                hbuf.at[q, chunk, r],
                size_send.at[2 + kind],
                ag_sem.at[legs.index(leg), q],
                ring_dev(q, step),
            ).start()

        sized(chunk, go)

    def ag_wait(leg, q):
        chunk = ring(q, -leg)
        sized(chunk, lambda r, kind: wait_bytes(hbuf.at[q, chunk, r], ag_sem.at[legs.index(leg), q]))

    def finish(q):
        rs_wait(fwd - 1, q, m)
        rs_wait(MSPLIT - 2, q, m)
        v = own[q, m] + rs_recv[fwd - 1, q].astype(F32) + rs_recv[MSPLIT - 2, q].astype(F32)
        v = v * factor
        ga = v[:, :LANES]
        up_half = v[:, LANES:]
        hbuf[q, m] = (ga / (1.0 + jnp.exp(-ga)) * up_half).astype(BF16)
        for leg in (2, -2, 1, -1):
            ag_start(leg, q, m, leg)

    each(pieces, finish)

    def relay(q):
        ag_wait(2, q)
        ag_start(4, q, ring(q, -2), 2)
        ag_start(3, q, ring(q, -2), 1)
        ag_wait(-2, q)
        ag_start(-3, q, ring(q, 2), -1)

    each(pieces, relay)

    loads[4].wait()
    col_iota = lax.broadcasted_iota(jnp.int32, (batch, rows), 1).astype(F32)
    row_iota = lax.broadcasted_iota(jnp.int32, (rows, LANES), 0)
    filled = lax.rem(row_iota, 2 * pad) < pad + short
    for e in range(RESIDENT):
        picks[e] = jnp.where(col_iota == cols_i[e], 1.0, 0.0).astype(BF16)
    acc[...] = jnp.zeros_like(acc)

    def down(q):
        for leg in (1, -1, 3, -3, 4):
            ag_wait(leg, q)
        units = pl.ds(pl.multiple_of(q * LANES, LANES), LANES)
        for e in range(RESIDENT):
            hc = hbuf[q, e * quarters : (e + 1) * quarters].astype(F32).reshape(rows, LANES)
            hc = jnp.where(filled, hc, 0.0).astype(BF16)
            spread = nn_dot(picks[e], hc).astype(BF16)
            acc[e] += nn_dot(spread, dwbuf[e, units, :])

    each(pieces, down)
    total = info[:, 0:1] * acc[0]
    for e in range(1, RESIDENT):
        total = total + info[:, e : e + 1] * acc[e]
    kout[...] = total.astype(BF16).reshape(hsplit, 8, bw)

    for step in patch_steps:
        j = patch_peer(step)
        copy_to(kout.at[j], kin.at[h], one_send.at[9], one_recv.at[7], m * hsplit + j).start()
    kin[h] = kout[h]
    wait_bytes(kin.at[pl.ds(0, hsplit - 1)], one_recv.at[7])
    ffn = kin[0].astype(F32)
    for j in range(1, hsplit):
        ffn = ffn + kin[j].astype(F32)
    final = resid_ref[...] + ffn
    for c in range(8):
        lf[pl.ds(c, 8, stride=8), :] = final[:, c * LANES : (c + 1) * LANES]
    lout[...] = lf[...].reshape(PLANE, 8, LANES).astype(BF16)

    def row_send(i):
        target = h * PLANE + i

        @pl.when(target != me)
        def _():
            copy_to(lout.at[i], lbuf.at[m], l_send.at[i], l_recv.at[m], target).start()

    each(PLANE, row_send)

    @pl.when(z == h)
    def _():
        lbuf[m] = lout[k]

    wait_bytes(abuf.at[0, pl.ds(0, PLANE - 1)], one_send.at[0])
    wait_bytes(wbuf.at[pl.ds(0, PLANE - 1)], one_send.at[1])
    wait_bytes(abuf.at[pl.ds(0, planes - 1)], one_send.at[2])
    wait_bytes(dbuf.at[pl.ds(0, hsplit - 1)], one_send.at[3])
    wait_bytes(meta_all.at[pl.ds(0, hsplit - 1)], one_send.at[4])
    wait_bytes(xbuf.at[pl.ds(0, hsplit - 1)], one_send.at[5])
    wait_bytes(ssq_all.at[pl.ds(0, MSPLIT - 1)], one_send.at[6])
    for parity in range(2):

        @pl.when(lax.rem(m, 2) == parity)
        def _(parity=parity):
            rs_even = MSPLIT // 2 - (1 - parity)
            ag_steps = (0, 0, 0, 0, -2, -2, 2)
            ag_even = sum((parity + step) % 2 == 0 for step in ag_steps)
            wait_bytes(rs_send.at[pl.ds(0, rs_even)], size_send.at[0])
            wait_bytes(rs_send.at[pl.ds(0, hops - rs_even), :, pl.ds(0, short)], size_send.at[1])
            wait_bytes(hbuf.at[:, pl.ds(0, ag_even)], size_send.at[2])
            wait_bytes(hbuf.at[:, pl.ds(0, hops - ag_even), pl.ds(0, short)], size_send.at[3])

    wait_bytes(kin.at[pl.ds(0, hsplit - 1)], one_send.at[9])
    wait_bytes(route_all.at[pl.ds(0, hsplit - 1)], one_send.at[10])

    @pl.when(k != gatherer)
    def _():
        wait_bytes(sblk, st_send.at[0])
        wait_bytes(meta_out, me_send.at[0])

    @pl.when((k == gatherer) & (z == h))
    def _():
        wait_bytes(pst.at[pl.ds(0, MSPLIT - 1)], st_send.at[1])
        wait_bytes(route_all.at[pl.ds(0, MSPLIT - 1)], me_send.at[1])

    @pl.when((k == gatherer) & (z != h))
    def _():
        wait_bytes(pst, st_send.at[1])
        wait_bytes(route_all.at[pl.ds(0, MSPLIT)], me_send.at[1])

    def drain(j):
        @pl.when(j * hsplit + z != me)
        def _():
            wait_bytes(lbuf.at[j], l_recv.at[j])

        @pl.when(h * PLANE + j != me)
        def _():
            wait_bytes(lout.at[j], l_send.at[j])

    each(MSPLIT, drain)

    qf[...] = lbuf[...].reshape(MSPLIT * 8, LANES).astype(F32)
    for j in range(width // LANES):
        out_ref[0:1, j * LANES : (j + 1) * LANES] = qf[j : j + 1, :]


def on_device(
    stream_in,
    query,
    key_new,
    value_new,
    key_cache,
    value_cache,
    lengths,
    route_ids,
    route_scores,
    out_weight,
    norm_gain,
    gate_weight,
    up_weight,
    down_weight,
):
    n = lax.axis_size("gx")
    width = stream_in.shape[1]
    slots = key_cache.shape[1]
    kv = key_cache.shape[2]
    hidden = gate_weight.shape[2]
    bw = width // MSPLIT
    hsplit = n // MSPLIT
    planes = n // PLANE
    cols = out_weight.shape[1]
    quarters = MSPLIT // RESIDENT
    cap = 5 * n // 8
    edges = [-(-(cap * c // quarters) // 8) * 8 for c in range(quarters + 1)]
    pad = edges[1] - edges[0]
    short = edges[2] - edges[1]
    assert [b - a for a, b in zip(edges, edges[1:])] == [pad, short] * (quarters // 2)
    pieces = hidden // LANES
    cfg = dict(n=n, width=width, hidden=hidden, edges=edges, pad=pad, short=short)
    hops = MSPLIT - 1

    def vmem(*shape, dtype=BF16):
        return pltpu.VMEM(shape, dtype)

    scratch = [
        vmem(slots, kv),
        vmem(slots, kv),
        vmem(*gate_weight.shape),
        vmem(*up_weight.shape),
        vmem(*down_weight.shape),
        vmem(PLANE, cols, bw),
        vmem(width // LANES, LANES, dtype=F32),
        vmem(width // LANES, LANES, dtype=F32),
        vmem(MSPLIT, 8, LANES),
        vmem(KVH, 8, HS),
        vmem(planes, PLANE, 8, HS),
        vmem(n * 8, LANES, dtype=F32),
        vmem(hsplit, 8, PLANE * cols),
        vmem(hsplit, 8, PLANE * cols),
        vmem(PLANE, 8, LANES),
        vmem(1, LANES, dtype=F32),
        vmem(PLANE, 1, LANES, dtype=F32),
        vmem(8, LANES, dtype=F32),
        vmem(hsplit, 8, LANES, dtype=F32),
        vmem(8, bw, dtype=F32),
        vmem(8, bw),
        vmem(hsplit, 8, bw),
        vmem(1, LANES, dtype=F32),
        vmem(MSPLIT, 1, LANES, dtype=F32),
        vmem(RESIDENT, quarters * pad, bw),
        vmem(pieces, MSPLIT, pad, 2 * LANES, dtype=F32),
        vmem(hops, pieces, pad, 2 * LANES),
        vmem(hops, pieces, pad, 2 * LANES),
        vmem(pieces, MSPLIT, pad, LANES),
        vmem(hsplit, 8, bw),
        vmem(hsplit, 8, bw),
        vmem(PLANE * 8, LANES, dtype=F32),
        vmem(PLANE, 8, LANES),
        vmem(MSPLIT, 8, LANES),
        vmem(1, width),
        vmem(1, width),
        vmem(1, kv),
        vmem(1, kv),
        vmem(width // LANES, LANES, dtype=F32),
        pltpu.SMEM((1,), jnp.int32),
        pltpu.SMEM((1, 2), jnp.int32),
        pltpu.SMEM((1, 2), F32),
        vmem(MSPLIT, PLANE, 8, LANES),
        vmem(PLANE, 1, LANES, dtype=F32),
        vmem(8, LANES, dtype=F32),
        vmem(hsplit, 8, LANES, dtype=F32),
        vmem(RESIDENT, n, bw, dtype=F32),
        vmem(RESIDENT, n, quarters * pad),
        vmem(cols, width),
        pltpu.SemaphoreType.DMA((14,)),
        pltpu.SemaphoreType.DMA((11,)),
        pltpu.SemaphoreType.DMA((9,)),
        pltpu.SemaphoreType.DMA((planes,)),
        pltpu.SemaphoreType.REGULAR((4,)),
        pltpu.SemaphoreType.DMA((4,)),
        pltpu.SemaphoreType.DMA((2,)),
        pltpu.SemaphoreType.DMA((2,)),
        pltpu.SemaphoreType.DMA((2,)),
        pltpu.SemaphoreType.DMA((2,)),
        pltpu.SemaphoreType.DMA((hops, pieces)),
        pltpu.SemaphoreType.DMA((hops, pieces)),
        pltpu.SemaphoreType.DMA((PLANE,)),
        pltpu.SemaphoreType.DMA((MSPLIT,)),
    ]
    local = pl.BlockSpec(memory_space=pltpu.VMEM)
    anywhere = pl.BlockSpec(memory_space=pl.ANY)
    return pl.pallas_call(
        functools.partial(layer_kernel, cfg),
        out_shape=jax.ShapeDtypeStruct((1, width), F32),
        in_specs=[anywhere] * 14,
        out_specs=local,
        scratch_shapes=scratch,
        compiler_params=pltpu.CompilerParams(
            collective_id=0, has_side_effects=True, vmem_limit_bytes=60 * 1024 * 1024
        ),
        name="layer",
    )(
        lengths,
        route_ids,
        route_scores,
        stream_in,
        query,
        key_new,
        value_new,
        norm_gain.reshape(width // LANES, LANES),
        key_cache.reshape(slots, kv),
        value_cache.reshape(slots, kv),
        out_weight.T,
        gate_weight,
        up_weight,
        down_weight,
    ).astype(BF16)


def solution(mesh):
    rows = P(("groups", "gx"), None)
    in_specs = (
        rows,
        rows,
        rows,
        rows,
        P(("groups", "gx"), None, None),
        P(("groups", "gx"), None, None),
        P(("groups", "gx")),
        rows,
        rows,
        P(None, "gx"),
        P(),
        P(None, "gx", None),
        P(None, "gx", None),
        P(None, "gx", None),
    )
    return jax.shard_map(
        on_device, mesh=mesh, in_specs=in_specs, out_specs=rows, check_vma=False
    )
```

```python
import functools

import jax
import jax.numpy as jnp
from jax import lax
from jax.experimental import pallas as pl
from jax.experimental.pallas import tpu as pltpu
from jax.sharding import PartitionSpec as P

NH = 64
KVH = 8
HS = 128
RESIDENT = 2
MSPLIT = 8
PLANE = 8
LANES = 128
BF16 = jnp.bfloat16
F32 = jnp.float32
MESH = pl.DeviceIdType.MESH


def nt_dot(a, b):
    return lax.dot_general(a, b, (((1,), (1,)), ((), ())), preferred_element_type=F32)


def nn_dot(a, b):
    return lax.dot_general(a, b, (((1,), (0,)), ((), ())), preferred_element_type=F32)


def copy_to(src, dst, send, recv, target):
    return pltpu.make_async_remote_copy(
        src_ref=src,
        dst_ref=dst,
        send_sem=send,
        recv_sem=recv,
        device_id={"gx": target},
        device_id_type=MESH,
    )


def wait_bytes(ref, sem):
    pltpu.make_async_copy(ref, ref, sem).wait()


def each(count, body, start=0):
    def step(i, carry):
        body(i)
        return carry

    lax.fori_loop(start, count, step, 0)


def layer_kernel(
    cfg,
    lengths_in,
    ids_in,
    scores_in,
    stream_in,
    query,
    key_new,
    value_new,
    gain,
    key_cache,
    value_cache,
    out_weight,
    gate_weight,
    up_weight,
    down_weight,
    out_ref,
    kbuf,
    vbuf,
    gbuf,
    ubuf,
    dwbuf,
    wbuf,
    qf,
    sf,
    sblk,
    att,
    abuf,
    af,
    pbuf,
    dbuf,
    sbuf,
    meta_out,
    meta_in,
    meta_blk,
    meta_all,
    resid_ref,
    yblk,
    xbuf,
    ssq_row,
    ssq_all,
    xcs,
    own,
    rs_send,
    rs_recv,
    hbuf,
    kout,
    kin,
    lf,
    lout,
    lbuf,
    svm,
    qvm,
    knvm,
    vnvm,
    gainvm,
    lengths,
    route_ids,
    route_scores,
    pst,
    pme,
    route_blk,
    route_all,
    acc,
    picks,
    wvm,
    loc_sem,
    one_send,
    one_recv,
    z_recv,
    tok,
    size_send,
    st_send,
    st_recv,
    me_send,
    me_recv,
    rs_sem,
    ag_sem,
    l_send,
    l_recv,
):
    n = cfg["n"]
    hsplit = n // MSPLIT
    planes = n // PLANE
    batch = n
    width = cfg["width"]
    bw = width // MSPLIT
    pieces = cfg["hidden"] // LANES
    edges = cfg["edges"]
    pad = cfg["pad"]
    short = cfg["short"]
    quarters = MSPLIT // RESIDENT
    rows = quarters * pad
    hops = MSPLIT - 1

    me = lax.axis_index("gx")
    z = me // PLANE
    k = lax.rem(me, PLANE)
    m = me // hsplit
    h = lax.rem(me, hsplit)
    low = me - m * hsplit
    sgn = 1 - 2 * lax.rem(me, 2)

    def up(step):
        return lax.rem(z + sgn * step + 2 * planes, planes)

    def signal(sem, target):
        pl.semaphore_signal(sem, inc=1, device_id={"gx": target}, device_id_type=MESH)

    small = [
        pltpu.make_async_copy(src, dst, loc_sem.at[6 + i])
        for i, (src, dst) in enumerate(
            [
                (query, qvm),
                (key_new, knvm),
                (value_new, vnvm),
                (lengths_in, lengths),
                (stream_in, svm),
                (gain, gainvm),
                (ids_in, route_ids),
                (scores_in, route_scores),
            ]
        )
    ]
    for load in small:
        load.start()
    loads = [
        pltpu.make_async_copy(key_cache, kbuf, loc_sem.at[0]),
        pltpu.make_async_copy(value_cache, vbuf, loc_sem.at[1]),
        pltpu.make_async_copy(gate_weight, gbuf, loc_sem.at[2]),
        pltpu.make_async_copy(up_weight, ubuf, loc_sem.at[3]),
        pltpu.make_async_copy(down_weight, dwbuf, loc_sem.at[4]),
        pltpu.make_async_copy(out_weight, wvm, loc_sem.at[5]),
    ]
    for load in loads[:2]:
        load.start()

    xs = k // 2
    core = lax.rem(k, 2)

    def peer(dx, dc):
        return 2 * lax.rem(xs + dx, PLANE // 2) + lax.rem(core + dc, 2)

    plane_steps = [(dx, dc) for dx in (2, 3, 1) for dc in (0, 1)] + [(0, 1)]
    patch_steps = [(dz, dx, dc) for dx in (2, 3, 1) for dz in (1, 0) for dc in (0, 1)]
    patch_steps += [(1, 0, 0), (1, 0, 1), (0, 0, 1)]

    def patch_peer(step):
        dz, dx, dc = step
        return lax.rem(h // PLANE + dz, 2) * PLANE + peer(dx, dc)

    barrier = pltpu.get_barrier_semaphore()

    for step in (1, -1):
        signal(barrier, up(step) * PLANE + k)

    def greet(i):
        signal(barrier, z * PLANE + lax.rem(k + i, PLANE))

    each(PLANE, greet, 1)

    loads[5].start()
    for load in loads[2:5]:
        load.start()

    for load in small[:4]:
        load.wait()
    for j in range(width // LANES):
        qf[j : j + 1, :] = qvm[0:1, j * LANES : (j + 1) * LANES].astype(F32)

    def per_group(row_ref):
        return jnp.concatenate(
            [
                jnp.broadcast_to(row_ref[0:1, g * HS : (g + 1) * HS].astype(F32), (NH // KVH, HS))
                for g in range(KVH)
            ],
            axis=0,
        )

    q_all = qf[...]
    scale = HS ** (-0.5)
    o = jnp.sum(q_all * per_group(knvm), axis=1, keepdims=True) * scale
    v_own = per_group(vnvm)
    loads[0].wait()
    slots = kbuf.shape[0]
    s = jnp.concatenate(
        [
            nt_dot(q_all[g * 8 : (g + 1) * 8].astype(BF16), kbuf[:, g * HS : (g + 1) * HS])
            for g in range(KVH)
        ],
        axis=0,
    )
    live = lax.broadcasted_iota(jnp.int32, (NH, slots), 1) < lengths[0]
    s = jnp.where(live, s * scale, -1e30)
    t = jnp.maximum(jnp.max(s, axis=1, keepdims=True), o)
    es = jnp.exp(s - t)
    eo = jnp.exp(o - t)
    total = jnp.sum(es, axis=1, keepdims=True) + eo
    p = es / total
    own_term = (eo / total).astype(BF16).astype(F32) * v_own
    loads[1].wait()
    for g in range(KVH):
        r = slice(g * 8, (g + 1) * 8)
        mixed = nn_dot(p[r].astype(BF16), vbuf[:, g * HS : (g + 1) * HS])
        att[g] = (mixed + own_term[r]).astype(BF16)

    pl.semaphore_wait(barrier, PLANE + 1)
    for step in (1, -1):
        signal(tok.at[0], up(step) * PLANE + k)

    for step in plane_steps:
        j = peer(*step)
        copy_to(
            att.at[j], abuf.at[z, k], one_send.at[0], one_recv.at[0], z * PLANE + j
        ).start()

    abuf[z, k] = att[k]
    for step in plane_steps:
        signal(tok.at[3], z * PLANE + peer(*step))

    for load in small[4:]:
        load.wait()
    for j in range(width // LANES):
        sf[j : j + 1, :] = svm[0:1, j * LANES : (j + 1) * LANES].astype(F32)
    sblk[...] = sf[...].reshape(MSPLIT, 8, LANES).astype(BF16)
    lane = lax.broadcasted_iota(jnp.int32, (1, LANES), 1)
    s0 = jnp.full((1, LANES), route_scores[0, 0], F32)
    s1 = jnp.full((1, LANES), route_scores[0, 1], F32)
    top = jnp.maximum(s0, s1)
    e0 = jnp.exp(s0 - top)
    e1 = jnp.exp(s1 - top)
    q0 = e0 / (e0 + e1)
    q1 = e1 / (e0 + e1)
    id0 = jnp.full((1, LANES), route_ids[0, 0], jnp.int32)
    id1 = jnp.full((1, LANES), route_ids[0, 1], jnp.int32)
    meta = jnp.zeros((1, LANES), F32)
    for e in range(RESIDENT):
        w = jnp.where(id0 == e, q0, 0.0) + jnp.where(id1 == e, q1, 0.0)
        w = w.astype(BF16).astype(F32)
        picked = jnp.where((id0 == e) | (id1 == e), 1.0, 0.0)
        meta = jnp.where(lane == e, w, meta)
        meta = jnp.where(lane == RESIDENT + e, picked, meta)
    meta_out[...] = meta

    gatherer = lax.rem(z, PLANE)

    @pl.when(k != gatherer)
    def _():
        target = z * PLANE + gatherer
        copy_to(sblk, pst.at[:, k], st_send.at[0], st_recv.at[0], target).start()
        copy_to(meta_out, pme.at[k], me_send.at[0], me_recv.at[0], target).start()

    @pl.when(k == gatherer)
    def _():
        for j in range(MSPLIT):
            pst[j, k] = sblk[j]
        pme[k] = meta_out[...]

    loads[5].wait()
    pl.semaphore_wait(tok.at[3], PLANE - 1)
    for step in sorted(plane_steps, key=lambda step: step[0] == 2):
        j = peer(*step)
        copy_to(
            wvm.at[:, pl.ds(pl.multiple_of(j * bw, bw), bw)],
            wbuf.at[k],
            one_send.at[1],
            one_recv.at[1],
            z * PLANE + j,
        ).start()

    pl.semaphore_wait(tok.at[0], 2)
    for step in (2, -2):
        signal(tok.at[1], up(step) * PLANE + k)

    wait_bytes(abuf.at[0, pl.ds(0, PLANE - 1)], one_recv.at[0])
    pl.semaphore_wait(tok.at[1], 2)

    def z_copy(origin, step):
        return copy_to(
            abuf.at[origin],
            abuf.at[origin],
            one_send.at[2],
            z_recv.at[origin],
            up(step) * PLANE + k,
        )

    reach = planes // 4
    for step in range(reach, 0, -1):
        z_copy(z, step).start()
        z_copy(z, -step).start()
    for step in (reach, -reach):
        signal(tok.at[2], up(step) * PLANE + k)
    @pl.when(k == gatherer)
    def _():
        pl.semaphore_wait(tok.at[2], 2)
        wait_bytes(pst.at[pl.ds(0, PLANE - 1)], st_recv.at[0])
        wait_bytes(pme.at[pl.ds(0, PLANE - 1)], me_recv.at[0])

        def hand_on(j):
            target = j * hsplit + z

            @pl.when(target != me)
            def _():
                copy_to(pst.at[j], sbuf, st_send.at[1], st_recv.at[1], target).start()
                copy_to(pme, meta_in, me_send.at[1], me_recv.at[1], target).start()

            @pl.when(target == me)
            def _():
                sbuf[...] = pst[j]
                meta_in[...] = pme[...]

        each(MSPLIT, hand_on)

    far = up(-reach)
    wait_bytes(abuf.at[far], z_recv.at[far])
    for step in range(reach, 0, -1):
        z_copy(far, step).start()
    near = up(reach)
    wait_bytes(abuf.at[near], z_recv.at[near])
    for step in range(reach - 1, 0, -1):
        z_copy(near, -step).start()
    @pl.when(k != gatherer)
    def _():
        pl.semaphore_wait(tok.at[2], 2)

    def z_wait(i):
        origin = lax.rem(z + i, planes)

        @pl.when((origin != far) & (origin != near))
        def _():
            wait_bytes(abuf.at[origin], z_recv.at[origin])

    each(planes, z_wait, 1)

    wbuf[k] = wvm[:, pl.ds(pl.multiple_of(k * bw, bw), bw)]
    wait_bytes(wbuf.at[pl.ds(0, PLANE - 1)], one_recv.at[1])

    af[...] = abuf[...].reshape(batch * 8, LANES).astype(F32)
    a = jnp.concatenate(
        [af[pl.ds(j, batch, stride=8), :] for j in range(8)], axis=1
    ).astype(BF16)
    part = nt_dot(a, wbuf[...].reshape(PLANE * wbuf.shape[1], bw))
    pbuf[...] = part.astype(BF16).reshape(hsplit, 8, part.shape[1])

    for step in patch_steps:
        j = patch_peer(step)
        copy_to(pbuf.at[j], dbuf.at[h], one_send.at[3], one_recv.at[3], m * hsplit + j).start()
    dbuf[h] = pbuf[h]

    @pl.when(z != h)
    def _():
        wait_bytes(sbuf, st_recv.at[1])
        wait_bytes(meta_in, me_recv.at[1])

    route_blk[...] = jnp.concatenate([meta_in[i] for i in range(PLANE)], axis=0)
    route_all[h] = route_blk[...]
    for step in patch_steps:
        target = m * hsplit + patch_peer(step)
        copy_to(route_blk, route_all.at[h], one_send.at[10], one_recv.at[8], target).start()
    lf[...] = sbuf[...].reshape(PLANE * 8, LANES).astype(F32)
    stream = jnp.concatenate([lf[pl.ds(c, 8, stride=8), :] for c in range(8)], axis=1)
    g8 = gainvm[pl.ds(pl.multiple_of(m * 8, 8), 8), :]
    gain_row = jnp.concatenate([g8[c : c + 1, :] for c in range(8)], axis=1)

    wait_bytes(dbuf.at[pl.ds(0, hsplit - 1)], one_recv.at[3])
    halves = []
    for half in range(hsplit // PLANE):
        part_sum = dbuf[half * PLANE].astype(F32)
        for j in range(1, PLANE):
            part_sum = part_sum + dbuf[half * PLANE + j].astype(F32)
        halves.append(part_sum)
    proj = jnp.concatenate(halves, axis=1).astype(BF16).astype(F32)
    resid = stream + proj
    resid_ref[...] = resid
    yblk[...] = (resid * gain_row).astype(BF16)
    xbuf[h] = yblk[...]
    for step in patch_steps:
        target = m * hsplit + patch_peer(step)
        copy_to(yblk, xbuf.at[h], one_send.at[5], one_recv.at[5], target).start()
    ssq = jnp.sum(resid * resid, axis=1, keepdims=True)
    row8 = lax.broadcasted_iota(jnp.int32, (8, LANES), 0)
    lane8 = lax.broadcasted_iota(jnp.int32, (8, LANES), 1)
    meta_blk[...] = jnp.sum(jnp.where(lane8 == h * 8 + row8, ssq, 0.0), axis=0, keepdims=True)
    meta_all[h] = meta_blk[...]
    for step in patch_steps:
        target = m * hsplit + patch_peer(step)
        copy_to(meta_blk, meta_all.at[h], one_send.at[4], one_recv.at[4], target).start()

    wait_bytes(route_all.at[pl.ds(0, hsplit - 1)], one_recv.at[8])
    info = route_all[...].reshape(batch, LANES)
    info_t = info.T
    ia = lax.broadcasted_iota(jnp.int32, (batch, batch), 0)
    ib = lax.broadcasted_iota(jnp.int32, (batch, batch), 1)
    before_t = jnp.where(ia < ib, 1.0, 0.0).astype(BF16)
    before = jnp.where(ib < ia, 1.0, 0.0).astype(BF16)
    ranks_t = nn_dot(info_t[0:8].astype(BF16), before_t)
    ranks = nn_dot(before, info.astype(BF16))

    def place_of(rank, picked):
        out = rank
        for c in range(1, quarters):
            step = float(c * pad - edges[c] - (c - 1) * pad + edges[c - 1])
            if step:
                out = out + jnp.where(rank >= float(edges[c]), step, 0.0)
        return jnp.where(picked > 0.5, out, -1.0)

    rows_i = [place_of(ranks_t[RESIDENT + e : RESIDENT + e + 1], info_t[RESIDENT + e : RESIDENT + e + 1]) for e in range(RESIDENT)]
    cols_i = [place_of(ranks[:, RESIDENT + e : RESIDENT + e + 1], info[:, RESIDENT + e : RESIDENT + e + 1]) for e in range(RESIDENT)]
    wait_bytes(xbuf.at[pl.ds(0, hsplit - 1)], one_recv.at[5])
    x = xbuf[...].reshape(batch, bw)
    r_iota = lax.broadcasted_iota(jnp.int32, (rows, batch), 0).astype(F32)
    for e in range(RESIDENT):
        pick = jnp.where(r_iota == rows_i[e], 1.0, 0.0).astype(BF16)
        xcs[e] = nn_dot(pick, x).astype(BF16)
    loads[2].wait()
    loads[3].wait()

    fwd = MSPLIT // 2
    bwd = MSPLIT - 1 - fwd

    def ring(q, step):
        turn = sgn * (1 - 2 * (q // fwd))
        return lax.rem(m + turn * step + 2 * MSPLIT, MSPLIT)

    def ring_dev(q, step):
        return ring(q, step) * hsplit + low

    def sized(chunk, body):
        odd = lax.rem(chunk, 2)

        @pl.when(odd == 0)
        def _():
            body(pl.ds(0, pad), 0)

        @pl.when(odd == 1)
        def _():
            body(pl.ds(0, short), 1)

    def rs_start(slot, q, chunk, target):
        def go(r, kind):
            copy_to(
                rs_send.at[slot, q, r],
                rs_recv.at[slot, q, r],
                size_send.at[kind],
                rs_sem.at[slot, q],
                target,
            ).start()

        sized(chunk, go)

    def rs_wait(slot, q, chunk):
        sized(chunk, lambda r, kind: wait_bytes(rs_recv.at[slot, q, r], rs_sem.at[slot, q]))

    def first(q):
        cols = pl.ds(pl.multiple_of(q * LANES, LANES), LANES)
        for e in range(RESIDENT):
            rhs = jnp.concatenate([gbuf[e, :, cols], ubuf[e, :, cols]], axis=1)
            r = nn_dot(xcs[e], rhs)
            own[q, e * quarters : (e + 1) * quarters] = r.reshape(quarters, pad, 2 * LANES)
        rs_send[0, q] = own[q, ring(q, fwd)].astype(BF16)
        rs_start(0, q, ring(q, fwd), ring_dev(q, 1))
        rs_send[fwd, q] = own[q, ring(q, -bwd)].astype(BF16)
        rs_start(fwd, q, ring(q, -bwd), ring_dev(q, -1))

    each(pieces, first)

    wait_bytes(meta_all.at[pl.ds(0, hsplit - 1)], one_recv.at[4])
    block_sum = meta_all[0]
    for j in range(1, hsplit):
        block_sum = block_sum + meta_all[j]
    ssq_row[...] = block_sum
    ssq_all[m] = ssq_row[...]

    def ssq_send(i):
        j = lax.rem(m + i, MSPLIT)
        copy_to(ssq_row, ssq_all.at[m], one_send.at[6], one_recv.at[6], j * hsplit + low).start()

    each(MSPLIT, ssq_send, 1)

    for t in range(1, fwd):

        def onward(q, t=t):
            chunk = ring(q, fwd - t)
            rs_wait(t - 1, q, chunk)
            v = rs_recv[t - 1, q].astype(F32) + own[q, chunk]
            rs_send[t, q] = v.astype(BF16)
            rs_start(t, q, chunk, ring_dev(q, 1))
            if t < bwd:
                b = fwd + t
                chunk = ring(q, t - bwd)
                rs_wait(b - 1, q, chunk)
                v = rs_recv[b - 1, q].astype(F32) + own[q, chunk]
                rs_send[b, q] = v.astype(BF16)
                rs_start(b, q, chunk, ring_dev(q, -1))

        each(pieces, onward)

    wait_bytes(ssq_all.at[pl.ds(0, MSPLIT - 1)], one_recv.at[6])
    power = ssq_all[0]
    for j in range(1, MSPLIT):
        power = power + ssq_all[j]
    chunk_row = jnp.where(m < quarters, rows_i[0], rows_i[1])
    c_iota = lax.broadcasted_iota(jnp.int32, (pad, batch), 0) + lax.rem(m, quarters) * pad
    hit = c_iota.astype(F32) == chunk_row
    mean = jnp.sum(jnp.where(hit, power, 0.0), axis=1, keepdims=True) / float(width)
    factor = lax.rsqrt(mean + 1e-05)

    legs = (1, 2, 3, 4, -1, -2, -3)

    def ag_start(leg, q, chunk, step):
        def go(r, kind):
            copy_to(
                hbuf.at[q, chunk, r],
                hbuf.at[q, chunk, r],
                size_send.at[2 + kind],
                ag_sem.at[legs.index(leg), q],
                ring_dev(q, step),
            ).start()

        sized(chunk, go)

    def ag_wait(leg, q):
        chunk = ring(q, -leg)
        sized(chunk, lambda r, kind: wait_bytes(hbuf.at[q, chunk, r], ag_sem.at[legs.index(leg), q]))

    def finish(q):
        rs_wait(fwd - 1, q, m)
        rs_wait(MSPLIT - 2, q, m)
        v = own[q, m] + rs_recv[fwd - 1, q].astype(F32) + rs_recv[MSPLIT - 2, q].astype(F32)
        v = v * factor
        ga = v[:, :LANES]
        up_half = v[:, LANES:]
        hbuf[q, m] = (ga / (1.0 + jnp.exp(-ga)) * up_half).astype(BF16)
        for leg in (2, -2, 1, -1):
            ag_start(leg, q, m, leg)

    each(pieces, finish)

    def relay(q):
        ag_wait(2, q)
        ag_start(4, q, ring(q, -2), 2)
        ag_start(3, q, ring(q, -2), 1)
        ag_wait(-2, q)
        ag_start(-3, q, ring(q, 2), -1)

    each(pieces, relay)

    loads[4].wait()
    col_iota = lax.broadcasted_iota(jnp.int32, (batch, rows), 1).astype(F32)
    row_iota = lax.broadcasted_iota(jnp.int32, (rows, LANES), 0)
    filled = lax.rem(row_iota, 2 * pad) < pad + short
    for e in range(RESIDENT):
        picks[e] = jnp.where(col_iota == cols_i[e], 1.0, 0.0).astype(BF16)
    acc[...] = jnp.zeros_like(acc)

    def down(q):
        for leg in (1, -1, 3, -3, 4):
            ag_wait(leg, q)
        units = pl.ds(pl.multiple_of(q * LANES, LANES), LANES)
        for e in range(RESIDENT):
            hc = hbuf[q, e * quarters : (e + 1) * quarters].astype(F32).reshape(rows, LANES)
            hc = jnp.where(filled, hc, 0.0).astype(BF16)
            spread = nn_dot(picks[e], hc).astype(BF16)
            acc[e] += nn_dot(spread, dwbuf[e, units, :])

    each(pieces, down)
    total = info[:, 0:1] * acc[0]
    for e in range(1, RESIDENT):
        total = total + info[:, e : e + 1] * acc[e]
    kout[...] = total.astype(BF16).reshape(hsplit, 8, bw)

    for step in patch_steps:
        j = patch_peer(step)
        copy_to(kout.at[j], kin.at[h], one_send.at[9], one_recv.at[7], m * hsplit + j).start()
    kin[h] = kout[h]
    wait_bytes(kin.at[pl.ds(0, hsplit - 1)], one_recv.at[7])
    ffn = kin[0].astype(F32)
    for j in range(1, hsplit):
        ffn = ffn + kin[j].astype(F32)
    final = resid_ref[...] + ffn
    for c in range(8):
        lf[pl.ds(c, 8, stride=8), :] = final[:, c * LANES : (c + 1) * LANES]
    lout[...] = lf[...].reshape(PLANE, 8, LANES).astype(BF16)

    def row_send(i):
        target = h * PLANE + i

        @pl.when(target != me)
        def _():
            copy_to(lout.at[i], lbuf.at[m], l_send.at[i], l_recv.at[m], target).start()

    each(PLANE, row_send)

    @pl.when(z == h)
    def _():
        lbuf[m] = lout[k]

    wait_bytes(abuf.at[0, pl.ds(0, PLANE - 1)], one_send.at[0])
    wait_bytes(wbuf.at[pl.ds(0, PLANE - 1)], one_send.at[1])
    wait_bytes(abuf.at[pl.ds(0, planes - 1)], one_send.at[2])
    wait_bytes(dbuf.at[pl.ds(0, hsplit - 1)], one_send.at[3])
    wait_bytes(meta_all.at[pl.ds(0, hsplit - 1)], one_send.at[4])
    wait_bytes(xbuf.at[pl.ds(0, hsplit - 1)], one_send.at[5])
    wait_bytes(ssq_all.at[pl.ds(0, MSPLIT - 1)], one_send.at[6])
    for parity in range(2):

        @pl.when(lax.rem(m, 2) == parity)
        def _(parity=parity):
            rs_even = MSPLIT // 2 - (1 - parity)
            ag_steps = (0, 0, 0, 0, -2, -2, 2)
            ag_even = sum((parity + step) % 2 == 0 for step in ag_steps)
            wait_bytes(rs_send.at[pl.ds(0, rs_even)], size_send.at[0])
            wait_bytes(rs_send.at[pl.ds(0, hops - rs_even), :, pl.ds(0, short)], size_send.at[1])
            wait_bytes(hbuf.at[:, pl.ds(0, ag_even)], size_send.at[2])
            wait_bytes(hbuf.at[:, pl.ds(0, hops - ag_even), pl.ds(0, short)], size_send.at[3])

    wait_bytes(kin.at[pl.ds(0, hsplit - 1)], one_send.at[9])
    wait_bytes(route_all.at[pl.ds(0, hsplit - 1)], one_send.at[10])

    @pl.when(k != gatherer)
    def _():
        wait_bytes(sblk, st_send.at[0])
        wait_bytes(meta_out, me_send.at[0])

    @pl.when((k == gatherer) & (z == h))
    def _():
        wait_bytes(pst.at[pl.ds(0, MSPLIT - 1)], st_send.at[1])
        wait_bytes(route_all.at[pl.ds(0, MSPLIT - 1)], me_send.at[1])

    @pl.when((k == gatherer) & (z != h))
    def _():
        wait_bytes(pst, st_send.at[1])
        wait_bytes(route_all.at[pl.ds(0, MSPLIT)], me_send.at[1])

    def drain(j):
        @pl.when(j * hsplit + z != me)
        def _():
            wait_bytes(lbuf.at[j], l_recv.at[j])

        @pl.when(h * PLANE + j != me)
        def _():
            wait_bytes(lout.at[j], l_send.at[j])

    each(MSPLIT, drain)

    qf[...] = lbuf[...].reshape(MSPLIT * 8, LANES).astype(F32)
    for j in range(width // LANES):
        out_ref[0:1, j * LANES : (j + 1) * LANES] = qf[j : j + 1, :]


def on_device(
    stream_in,
    query,
    key_new,
    value_new,
    key_cache,
    value_cache,
    lengths,
    route_ids,
    route_scores,
    out_weight,
    norm_gain,
    gate_weight,
    up_weight,
    down_weight,
):
    n = lax.axis_size("gx")
    width = stream_in.shape[1]
    slots = key_cache.shape[1]
    kv = key_cache.shape[2]
    hidden = gate_weight.shape[2]
    bw = width // MSPLIT
    hsplit = n // MSPLIT
    planes = n // PLANE
    cols = out_weight.shape[1]
    quarters = MSPLIT // RESIDENT
    cap = 5 * n // 8
    edges = [-(-(cap * c // quarters) // 8) * 8 for c in range(quarters + 1)]
    pad = edges[1] - edges[0]
    short = edges[2] - edges[1]
    assert [b - a for a, b in zip(edges, edges[1:])] == [pad, short] * (quarters // 2)
    pieces = hidden // LANES
    cfg = dict(n=n, width=width, hidden=hidden, edges=edges, pad=pad, short=short)
    hops = MSPLIT - 1

    def vmem(*shape, dtype=BF16):
        return pltpu.VMEM(shape, dtype)

    scratch = [
        vmem(slots, kv),
        vmem(slots, kv),
        vmem(*gate_weight.shape),
        vmem(*up_weight.shape),
        vmem(*down_weight.shape),
        vmem(PLANE, cols, bw),
        vmem(width // LANES, LANES, dtype=F32),
        vmem(width // LANES, LANES, dtype=F32),
        vmem(MSPLIT, 8, LANES),
        vmem(KVH, 8, HS),
        vmem(planes, PLANE, 8, HS),
        vmem(n * 8, LANES, dtype=F32),
        vmem(hsplit, 8, PLANE * cols),
        vmem(hsplit, 8, PLANE * cols),
        vmem(PLANE, 8, LANES),
        vmem(1, LANES, dtype=F32),
        vmem(PLANE, 1, LANES, dtype=F32),
        vmem(1, LANES, dtype=F32),
        vmem(hsplit, 1, LANES, dtype=F32),
        vmem(8, bw, dtype=F32),
        vmem(8, bw),
        vmem(hsplit, 8, bw),
        vmem(1, LANES, dtype=F32),
        vmem(MSPLIT, 1, LANES, dtype=F32),
        vmem(RESIDENT, quarters * pad, bw),
        vmem(pieces, MSPLIT, pad, 2 * LANES, dtype=F32),
        vmem(hops, pieces, pad, 2 * LANES),
        vmem(hops, pieces, pad, 2 * LANES),
        vmem(pieces, MSPLIT, pad, LANES),
        vmem(hsplit, 8, bw),
        vmem(hsplit, 8, bw),
        vmem(PLANE * 8, LANES, dtype=F32),
        vmem(PLANE, 8, LANES),
        vmem(MSPLIT, 8, LANES),
        vmem(1, width),
        vmem(1, width),
        vmem(1, kv),
        vmem(1, kv),
        vmem(width // LANES, LANES, dtype=F32),
        pltpu.SMEM((1,), jnp.int32),
        pltpu.SMEM((1, 2), jnp.int32),
        pltpu.SMEM((1, 2), F32),
        vmem(MSPLIT, PLANE, 8, LANES),
        vmem(PLANE, 1, LANES, dtype=F32),
        vmem(8, LANES, dtype=F32),
        vmem(hsplit, 8, LANES, dtype=F32),
        vmem(RESIDENT, n, bw, dtype=F32),
        vmem(RESIDENT, n, quarters * pad),
        vmem(cols, width),
        pltpu.SemaphoreType.DMA((14,)),
        pltpu.SemaphoreType.DMA((11,)),
        pltpu.SemaphoreType.DMA((9,)),
        pltpu.SemaphoreType.DMA((planes,)),
        pltpu.SemaphoreType.REGULAR((4,)),
        pltpu.SemaphoreType.DMA((4,)),
        pltpu.SemaphoreType.DMA((2,)),
        pltpu.SemaphoreType.DMA((2,)),
        pltpu.SemaphoreType.DMA((2,)),
        pltpu.SemaphoreType.DMA((2,)),
        pltpu.SemaphoreType.DMA((hops, pieces)),
        pltpu.SemaphoreType.DMA((hops, pieces)),
        pltpu.SemaphoreType.DMA((PLANE,)),
        pltpu.SemaphoreType.DMA((MSPLIT,)),
    ]
    local = pl.BlockSpec(memory_space=pltpu.VMEM)
    anywhere = pl.BlockSpec(memory_space=pl.ANY)
    return pl.pallas_call(
        functools.partial(layer_kernel, cfg),
        out_shape=jax.ShapeDtypeStruct((1, width), F32),
        in_specs=[anywhere] * 14,
        out_specs=local,
        scratch_shapes=scratch,
        compiler_params=pltpu.CompilerParams(
            collective_id=0, has_side_effects=True, vmem_limit_bytes=60 * 1024 * 1024
        ),
        name="layer",
    )(
        lengths,
        route_ids,
        route_scores,
        stream_in,
        query,
        key_new,
        value_new,
        norm_gain.reshape(width // LANES, LANES),
        key_cache.reshape(slots, kv),
        value_cache.reshape(slots, kv),
        out_weight.T,
        gate_weight,
        up_weight,
        down_weight,
    ).astype(BF16)


def solution(mesh):
    rows = P(("groups", "gx"), None)
    in_specs = (
        rows,
        rows,
        rows,
        rows,
        P(("groups", "gx"), None, None),
        P(("groups", "gx"), None, None),
        P(("groups", "gx")),
        rows,
        rows,
        P(None, "gx"),
        P(),
        P(None, "gx", None),
        P(None, "gx", None),
        P(None, "gx", None),
    )
    return jax.shard_map(
        on_device, mesh=mesh, in_specs=in_specs, out_specs=rows, check_vma=False
    )
```
